32 devices in a mesh: rep: 2 (over x), fsdp: 4 (over z), ep: 4 (over y, core).
Axes of the slice: x: 2, y: 2, z: 4, core: 2. Of those that a mesh axis runs over, the one named last changes fastest.
Arguments:
- tokens: bfloat16 [32768, 1024], P(('rep', 'fsdp', 'ep')), parts along dimension 0
- expert_idx: int32 [32768, 8], P(('rep', 'fsdp', 'ep')), parts along dimension 0
- gates: float32 [32768, 8], P(('rep', 'fsdp', 'ep')), parts along dimension 0
- w_gate: bfloat16 [32, 1024, 512], P('ep', 'fsdp')
- w_up: bfloat16 [32, 1024, 512], P('ep', 'fsdp')
- w_down: bfloat16 [32, 512, 1024], P('ep', None, 'fsdp')
Outputs:
- output: bfloat16 [32768, 1024], P(('rep', 'fsdp', 'ep')), parts along dimension 0
There are 2 independent parts. The reference program is written for one: setup_inputs(seed, part) draws one part's arguments, and reference() takes and returns one part's arrays. A program takes and returns all parts, laid end to end along the dimension named above; an argument that names none is the same for every part.
All inputs are finite; a program needn't handle non-finite values.
Results may differ from the reference program's by a relative error of at most 0.001.
Values are sent between devices in bfloat16 or wider.
A program may use at most 1 GiB of HBM per device.

```python
import jax
import jax.numpy as jnp
from jax import lax

TOK_DEV = 1024
D_MODEL = 1024
FFN = 512
EXPERTS = 32
TOP = 8
FSDP = 4
EP = 4

DEV_GROUP = FSDP * EP
TOK_GROUP = TOK_DEV * DEV_GROUP
CAP = min(TOK_DEV // 2, 4 * TOP * TOK_DEV // EXPERTS)


def draw_routing(route_key):
    key_hot, key_dev = jax.random.split(route_key)
    order_all = jax.random.permutation(key_hot, EXPERTS)
    cold_total = TOP * TOK_DEV - TOP * CAP
    cold_base = cold_total // (EXPERTS - TOP)
    cold_extra = cold_total - cold_base * (EXPERTS - TOP)
    counts = jnp.concatenate([
        jnp.full((TOP,), CAP, jnp.int32),
        cold_base + (jnp.arange(EXPERTS - TOP) < cold_extra).astype(jnp.int32)])

    def one_device(dev_key):
        key_cold, key_tok = jax.random.split(dev_key)
        cold_ids = order_all[TOP:][jax.random.permutation(key_cold, EXPERTS - TOP)]
        labels = jnp.concatenate([order_all[:TOP], cold_ids])
        expanded = jnp.repeat(labels, counts, total_repeat_length=TOP * TOK_DEV)
        choice_table = expanded.reshape(TOP, TOK_DEV).T
        return choice_table[jax.random.permutation(key_tok, TOK_DEV)]

    per_device = jax.vmap(one_device)(jax.random.split(key_dev, DEV_GROUP))
    return per_device.reshape(TOK_GROUP, TOP).astype(jnp.int32)


def setup_inputs(seed: int = 0, part: int = 0) -> dict:
    part_key = jax.random.fold_in(jax.random.key(seed), part)
    key_x, key_route, key_gate = jax.random.split(part_key, 3)
    key_wg, key_wu, key_wd = jax.random.split(jax.random.key(seed + 1), 3)
    tokens = jax.random.normal(key_x, (TOK_GROUP, D_MODEL), jnp.float32).astype(jnp.bfloat16)
    gates = jax.random.uniform(key_gate, (TOK_GROUP, TOP), jnp.float32, 0.4, 1.6) * TOP ** -0.5
    w_gate = (jax.random.normal(key_wg, (EXPERTS, D_MODEL, FFN), jnp.float32) * D_MODEL ** -0.5).astype(jnp.bfloat16)
    w_up = (jax.random.normal(key_wu, (EXPERTS, D_MODEL, FFN), jnp.float32) * D_MODEL ** -0.5).astype(jnp.bfloat16)
    w_down = (jax.random.normal(key_wd, (EXPERTS, FFN, D_MODEL), jnp.float32) * (1.5 * FFN ** -0.5)).astype(jnp.bfloat16)
    return {'tokens': tokens, 'expert_idx': draw_routing(key_route), 'gates': gates,
            'w_gate': w_gate, 'w_up': w_up, 'w_down': w_down}


def slot_table(flat_ids, flat_gates):
    pair_order = jnp.argsort(flat_ids, stable=True)
    sorted_ids = flat_ids[pair_order]
    expert_range = jnp.arange(EXPERTS, dtype=jnp.int32)
    first_pos = jnp.searchsorted(sorted_ids, expert_range, side='left')
    last_pos = jnp.searchsorted(sorted_ids, expert_range, side='right')
    slot_pos = first_pos[:, None] + jnp.arange(CAP)[None, :]
    filled = slot_pos < last_pos[:, None]
    pair_at = pair_order[jnp.minimum(slot_pos, TOK_DEV * TOP - 1)]
    tok_local = jnp.where(filled, pair_at // TOP, TOK_DEV)
    gate_at = jnp.where(filled, flat_gates[pair_at], 0.0)
    return tok_local, gate_at


def reference(tokens, expert_idx, gates, w_gate, w_up, w_down):
    dev_tok, dev_gate = jax.vmap(slot_table)(
        expert_idx.reshape(DEV_GROUP, TOK_DEV * TOP), gates.reshape(DEV_GROUP, TOK_DEV * TOP))
    offsets = (jnp.arange(DEV_GROUP) * TOK_DEV)[:, None, None]
    glob_tok = jnp.where(dev_tok < TOK_DEV, dev_tok + offsets, TOK_GROUP)
    glob_tok = jnp.transpose(glob_tok, (1, 0, 2)).reshape(EXPERTS, DEV_GROUP * CAP)
    glob_gate = jnp.transpose(dev_gate, (1, 0, 2)).reshape(EXPERTS, DEV_GROUP * CAP)

    def expert_step(y_acc, packed):
        tok_ids, gate_vals, gate_mat, up_mat, down_mat = packed
        rows = jnp.take(tokens, tok_ids, axis=0, mode='fill', fill_value=0)
        act_g = jnp.dot(rows, gate_mat, preferred_element_type=jnp.float32)
        act_u = jnp.dot(rows, up_mat, preferred_element_type=jnp.float32)
        hidden = (jax.nn.silu(act_g) * act_u).astype(jnp.bfloat16)
        expert_out = jnp.dot(hidden, down_mat, preferred_element_type=jnp.float32).astype(jnp.bfloat16)
        y_acc = y_acc.at[tok_ids].add(gate_vals[:, None] * expert_out.astype(jnp.float32), mode='drop')
        return y_acc, None

    y_acc, unused = lax.scan(expert_step, tokens.astype(jnp.float32),
                             (glob_tok, glob_gate, w_gate, w_up, w_down))
    return y_acc.astype(jnp.bfloat16)
```

```python
import functools

import jax
import jax.numpy as jnp
from jax import lax
from jax.experimental import pallas as pl
from jax.experimental.pallas import tpu as pltpu
from jax.sharding import PartitionSpec as P

MESH = pl.DeviceIdType.MESH
N_Z = 4
N_BLOCK = 2


def moe_kernel(x_hbm, ids_hbm, gates_hbm, wg_hbm, wu_hbm, wd_hbm, out_hbm,
               wg, wu, wd, toks, ids, gates, acc, from_core, from_y,
               own_sem, recv_z, recv_x, send_r, send_l, send_x,
               tok_send, tok_recv, meta_send, meta_recv,
               sum_send, sum_recv, credit, out_sem):
    r = lax.axis_index('rep')
    z = lax.axis_index('fsdp')
    p = lax.axis_index('ep')
    core = p % 2
    core_peer = p + 1 - 2 * core
    y_peer = (p + 2) % 4
    far_peer = (core_peer + 2) % 4
    n_local = wg_hbm.shape[0]
    n_packet = n_local // 2
    d_shard = wg_hbm.shape[1]
    n_tok = x_hbm.shape[0]
    block = n_tok // N_BLOCK

    hbm = (wg_hbm, wu_hbm, wd_hbm)

    def shard(t, e, s):
        start = pl.multiple_of(s * d_shard, d_shard)
        if t == 2:
            return wd.at[e, :, pl.ds(start, d_shard)]
        return (wg, wu)[t].at[e, pl.ds(start, d_shard), :]

    def remote(src, dst, send_sem, recv_sem, **where):
        return pltpu.make_async_remote_copy(src_ref=src, dst_ref=dst, send_sem=send_sem, recv_sem=recv_sem,
                                            device_id=where, device_id_type=MESH)

    def z_copy(t, k, s, right, own):
        e = 2 * k + r
        src = hbm[t].at[e] if own else shard(t, e, s)
        send = send_r if right else send_l
        to = (z + 1) % N_Z if right else (z + N_Z - 1) % N_Z
        return remote(src, shard(t, e, s), send.at[t, k, s], recv_z.at[t, k, s], fsdp=to)

    def x_copy(t, k, s):
        e = 2 * k + r
        return remote(shard(t, e, s), shard(t, e, s), send_x.at[t, k, s], recv_x.at[t, k, s], rep=1 - r)

    def x_arrival(t, k, s):
        e = 2 * k + 1 - r
        return remote(shard(t, e, s), shard(t, e, s), send_x.at[t, k, s], recv_x.at[t, k, s], rep=1 - r)

    def send_own(k):
        for t in range(3):
            @pl.when(z > 0)
            def _():
                z_copy(t, k, z, False, True).start()

            @pl.when(z < N_Z - 1)
            def _():
                z_copy(t, k, z, True, True).start()

    def event(k, dist, t):
        left = (z + N_Z - dist) % N_Z
        right = (z + dist) % N_Z

        @pl.when(z + dist < N_Z)
        def _():
            z_copy(t, k, right, False, False).wait_recv()

            @pl.when(z > 0)
            def _():
                z_copy(t, k, right, False, False).start()
            x_copy(t, k, right).start()

        @pl.when(z >= dist)
        def _():
            z_copy(t, k, left, True, False).wait_recv()

            @pl.when(z < N_Z - 1)
            def _():
                z_copy(t, k, left, True, False).start()
            x_copy(t, k, left).start()

    def wait_x(k):
        for dist in range(1, N_Z):
            for t in range(3):
                x_arrival(t, k, (z + dist) % N_Z).wait_recv()

    barrier = pltpu.get_barrier_semaphore()
    for peer in (core_peer, y_peer, far_peer):
        pl.semaphore_signal(barrier, inc=1, device_id={'ep': peer}, device_id_type=MESH)
    pl.semaphore_signal(barrier, inc=1, device_id={'rep': 1 - r}, device_id_type=MESH)

    @pl.when(z > 0)
    def _():
        pl.semaphore_signal(barrier, inc=1, device_id={'fsdp': (z + N_Z - 1) % N_Z}, device_id_type=MESH)

    @pl.when(z < N_Z - 1)
    def _():
        pl.semaphore_signal(barrier, inc=1, device_id={'fsdp': (z + 1) % N_Z}, device_id_type=MESH)

    own_w = [pltpu.make_async_copy(hbm[t].at[e], shard(t, e, z), own_sem.at[t, e])
             for e in range(n_local) for t in range(3)]
    own_x = pltpu.make_async_copy(x_hbm, toks.at[3], own_sem.at[3, 0])
    own_ids = pltpu.make_async_copy(ids_hbm, ids.at[3], own_sem.at[3, 1])
    own_gates = pltpu.make_async_copy(gates_hbm, gates.at[3], own_sem.at[3, 2])
    own_copies = own_w + [own_x, own_ids, own_gates]
    for copy in own_copies:
        copy.start()

    pl.semaphore_wait(barrier, 4 + (z + N_Z - 1) // N_Z + (2 * N_Z - 2 - z) // N_Z)

    meta = []
    for slot, peer in ((2, core_peer), (1, y_peer), (0, far_peer)):
        meta.append(remote(ids_hbm, ids.at[slot], meta_send.at[0, slot], meta_recv.at[0, slot], ep=peer))
        meta.append(remote(gates_hbm, gates.at[slot], meta_send.at[1, slot], meta_recv.at[1, slot], ep=peer))
    for copy in meta:
        copy.start()
    send_own(0)
    tok_core = remote(x_hbm, toks.at[2], tok_send.at[2], tok_recv.at[2], ep=core_peer)
    tok_y = remote(x_hbm, toks.at[1], tok_send.at[1], tok_recv.at[1], ep=y_peer)
    tok_far = remote(toks.at[1], toks.at[0], tok_send.at[0], tok_recv.at[0], ep=core_peer)
    tok_core.start()
    tok_y.start()
    send_own(1)

    def zero(i, carry):
        rows = pl.ds(pl.multiple_of(i % N_BLOCK * block, block), block)
        acc[i // N_BLOCK, rows, :] = jnp.zeros((block, acc.shape[2]), jnp.float32)
        return carry

    lax.fori_loop(0, 4 * N_BLOCK, zero, 0)

    for dist in range(1, N_Z):
        for t in range(3):
            event(0, dist, t)
    for copy in own_copies:
        copy.wait()
    tok_y.wait_recv()
    tok_far.start()
    for copy in meta:
        copy.wait_recv()
    tok_core.wait_recv()
    wait_x(0)
    tok_far.wait_recv()

    def place(i):
        far = i < 2 * N_BLOCK
        slot = jnp.where(far, i % 2, i // N_BLOCK)
        row = jnp.where(far, i // 2, i % N_BLOCK)
        return slot, row

    def compute(e, slot, row):
        rows = pl.ds(pl.multiple_of(row * block, block), block)
        x = toks[slot, rows, :]
        a = jnp.dot(x, wg[e], preferred_element_type=jnp.float32)
        b = jnp.dot(x, wu[e], preferred_element_type=jnp.float32)
        h = (a * jax.nn.sigmoid(a) * b).astype(jnp.bfloat16)
        o = jnp.dot(h, wd[e], preferred_element_type=jnp.float32).astype(jnp.bfloat16).astype(jnp.float32)
        expert = p * n_local + e
        chosen = jnp.where(ids[slot, :, rows] == expert, gates[slot, :, rows], 0.0)
        gate = jnp.sum(chosen, axis=0, keepdims=True)
        gate = jnp.broadcast_to(gate, (128, block)).T
        for c in range(acc.shape[2] // 128):
            cols = slice(c * 128, (c + 1) * 128)
            acc[slot, rows, cols] += jnp.where(gate > 0, gate * o[:, cols], 0.0)

    n_step = 4 * N_BLOCK * 2

    def packet(k, carry):
        @pl.when(k + 2 < n_packet)
        def _():
            send_own(k + 2)

        def step(i, carry):
            for j in range(9):
                @pl.when(i == j * n_step // 9)
                def _():
                    event(k + 1, j // 3 + 1, j % 3)
            slot, row = place(i // 2)
            compute(2 * k + i % 2, slot, row)
            return carry

        lax.fori_loop(0, n_step, step, 0)
        wait_x(k + 1)
        return carry

    lax.fori_loop(0, n_packet - 1, packet, 0)

    def block_of(ref, row):
        return ref.at[pl.ds(row * block, block), :]

    def to_core(slot, row):
        return remote(block_of(acc.at[slot], row), block_of(from_core, row),
                      sum_send.at[slot, row], sum_recv.at[slot, row], ep=core_peer)

    def to_y(row):
        return remote(block_of(acc.at[1], row), block_of(from_y, row),
                      sum_send.at[1, row], sum_recv.at[1, row], ep=y_peer)

    def last_step(i, carry):
        slot, row = place(i // 2)
        compute(2 * (n_packet - 1) + i % 2, slot, row)
        for n in range(N_BLOCK):
            @pl.when(i == 4 * n + 1)
            def _():
                to_core(0, n).start()

            @pl.when(i == 4 * n + 3)
            def _():
                to_core(0, n).wait_recv()
                rows = slice(n * block, (n + 1) * block)
                acc[1, rows, :] += from_core[rows, :]
                to_y(n).start()
                pl.semaphore_signal(credit.at[n], inc=1, device_id={'ep': core_peer}, device_id_type=MESH)

            @pl.when(i == 4 * N_BLOCK + 2 * n + 1)
            def _():
                pl.semaphore_wait(credit.at[n], 1)
                to_core(2, n).start()
        return carry

    lax.fori_loop(0, n_step, last_step, 0)

    outs = []
    for n in range(N_BLOCK):
        rows = slice(n * block, (n + 1) * block)
        to_core(2, n).wait_recv()
        to_y(n).wait_recv()
        y = toks[3, rows, :].astype(jnp.float32) + (acc[3, rows, :] + from_core[rows, :] + from_y[rows, :])
        toks[3, rows, :] = y.astype(jnp.bfloat16)
        copy = pltpu.make_async_copy(block_of(toks.at[3], n), block_of(out_hbm, n), out_sem.at[n])
        copy.start()
        outs.append(copy)

    for copy in meta + [tok_core, tok_y, tok_far]:
        copy.wait_send()
    for n in range(N_BLOCK):
        to_core(0, n).wait_send()
        to_y(n).wait_send()
        to_core(2, n).wait_send()

    def drain(k, carry):
        for t in range(3):
            @pl.when(z > 0)
            def _():
                z_copy(t, k, z, False, True).wait_send()

            @pl.when(z < N_Z - 1)
            def _():
                z_copy(t, k, z, True, True).wait_send()
            for dist in range(1, N_Z):
                left = (z + N_Z - dist) % N_Z
                right = (z + dist) % N_Z

                @pl.when((z + dist < N_Z) & (z > 0))
                def _():
                    z_copy(t, k, right, False, False).wait_send()

                @pl.when((z >= dist) & (z < N_Z - 1))
                def _():
                    z_copy(t, k, left, True, False).wait_send()
                x_copy(t, k, (z + dist) % N_Z).wait_send()
        return carry

    lax.fori_loop(0, n_packet, drain, 0)
    for copy in outs:
        copy.wait()


def solution(mesh):
    tok_spec = P(('rep', 'fsdp', 'ep'), None)

    def device_step(x_blk, ids_blk, gate_blk, wg_blk, wu_blk, wd_blk):
        n_tok, d_model = x_blk.shape
        n_choice = ids_blk.shape[1]
        n_local, d_shard, ffn = wg_blk.shape
        dma = pltpu.SemaphoreType.DMA
        n_packet = n_local // 2
        any_space = pl.BlockSpec(memory_space=pl.ANY)
        flops = 4 * n_tok * n_local * 6 * d_model * ffn
        return pl.pallas_call(
            moe_kernel,
            out_shape=jax.ShapeDtypeStruct((n_tok, d_model), jnp.bfloat16),
            in_specs=[any_space] * 6,
            out_specs=any_space,
            scratch_shapes=[
                pltpu.VMEM((n_local, d_model, ffn), jnp.bfloat16),
                pltpu.VMEM((n_local, d_model, ffn), jnp.bfloat16),
                pltpu.VMEM((n_local, ffn, d_model), jnp.bfloat16),
                pltpu.VMEM((4, n_tok, d_model), jnp.bfloat16),
                pltpu.VMEM((4, n_choice, n_tok), jnp.int32),
                pltpu.VMEM((4, n_choice, n_tok), jnp.float32),
                pltpu.VMEM((4, n_tok, d_model), jnp.float32),
                pltpu.VMEM((n_tok, d_model), jnp.float32),
                pltpu.VMEM((n_tok, d_model), jnp.float32),
                dma((4, n_local)),
                dma((3, n_packet, N_Z)),
                dma((3, n_packet, N_Z)),
                dma((3, n_packet, N_Z)),
                dma((3, n_packet, N_Z)),
                dma((3, n_packet, N_Z)),
                dma((3,)),
                dma((3,)),
                dma((2, 3)),
                dma((2, 3)),
                dma((3, N_BLOCK)),
                dma((3, N_BLOCK)),
                pltpu.SemaphoreType.REGULAR((N_BLOCK,)),
                dma((N_BLOCK,)),
            ],
            compiler_params=pltpu.CompilerParams(
                collective_id=0, has_side_effects=True, vmem_limit_bytes=67043328),
            cost_estimate=pl.CostEstimate(flops=flops, bytes_accessed=32 << 20, transcendentals=0),
            name='moe',
        )(x_blk, ids_blk.T, gate_blk.T, wg_blk, wu_blk, wd_blk)

    return jax.shard_map(
        device_step, mesh=mesh,
        in_specs=(tok_spec, tok_spec, tok_spec, P('ep', 'fsdp', None), P('ep', 'fsdp', None), P('ep', None, 'fsdp')),
        out_specs=tok_spec, check_vma=False)
```

```python
import functools

import jax
import jax.numpy as jnp
from jax import lax
from jax.experimental import pallas as pl
from jax.experimental.pallas import tpu as pltpu
from jax.sharding import PartitionSpec as P

MESH = pl.DeviceIdType.MESH
N_Z = 4
N_BLOCK = 2
N_TAIL = 4


def moe_kernel(x_hbm, ids_hbm, gates_hbm, wg_hbm, wu_hbm, wd_hbm, out_hbm,
               wg, wu, wd, toks, ids, gates, acc, from_core, from_y,
               own_sem, recv_z, recv_x, send_r, send_l, send_x,
               tok_send, tok_recv, meta_send, meta_recv,
               sum_send, sum_recv, credit, out_sem):
    r = lax.axis_index('rep')
    z = lax.axis_index('fsdp')
    p = lax.axis_index('ep')
    core = p % 2
    core_peer = p + 1 - 2 * core
    y_peer = (p + 2) % 4
    far_peer = (core_peer + 2) % 4
    n_local = wg_hbm.shape[0]
    n_packet = n_local // 2
    d_shard = wg_hbm.shape[1]
    n_tok = x_hbm.shape[0]
    block = n_tok // N_BLOCK

    hbm = (wg_hbm, wu_hbm, wd_hbm)

    def shard(t, e, s):
        start = pl.multiple_of(s * d_shard, d_shard)
        if t == 2:
            return wd.at[e, :, pl.ds(start, d_shard)]
        return (wg, wu)[t].at[e, pl.ds(start, d_shard), :]

    def remote(src, dst, send_sem, recv_sem, **where):
        return pltpu.make_async_remote_copy(src_ref=src, dst_ref=dst, send_sem=send_sem, recv_sem=recv_sem,
                                            device_id=where, device_id_type=MESH)

    def z_copy(t, k, s, right, own):
        e = 2 * k + r
        src = hbm[t].at[e] if own else shard(t, e, s)
        send = send_r if right else send_l
        to = (z + 1) % N_Z if right else (z + N_Z - 1) % N_Z
        return remote(src, shard(t, e, s), send.at[t, k, s], recv_z.at[t, k, s], fsdp=to)

    def x_copy(t, k, s):
        e = 2 * k + r
        return remote(shard(t, e, s), shard(t, e, s), send_x.at[t, k, s], recv_x.at[t, k, s], rep=1 - r)

    def x_arrival(t, k, s):
        e = 2 * k + 1 - r
        return remote(shard(t, e, s), shard(t, e, s), send_x.at[t, k, s], recv_x.at[t, k, s], rep=1 - r)

    def send_own(k):
        for t in range(3):
            @pl.when(z > 0)
            def _():
                z_copy(t, k, z, False, True).start()

            @pl.when(z < N_Z - 1)
            def _():
                z_copy(t, k, z, True, True).start()

    def event(k, dist, t):
        left = (z + N_Z - dist) % N_Z
        right = (z + dist) % N_Z

        @pl.when(z + dist < N_Z)
        def _():
            z_copy(t, k, right, False, False).wait_recv()

            @pl.when(z > 0)
            def _():
                z_copy(t, k, right, False, False).start()
            x_copy(t, k, right).start()

        @pl.when(z >= dist)
        def _():
            z_copy(t, k, left, True, False).wait_recv()

            @pl.when(z < N_Z - 1)
            def _():
                z_copy(t, k, left, True, False).start()
            x_copy(t, k, left).start()

    def wait_x(k):
        for dist in range(1, N_Z):
            for t in range(3):
                x_arrival(t, k, (z + dist) % N_Z).wait_recv()

    barrier = pltpu.get_barrier_semaphore()
    for peer in (core_peer, y_peer, far_peer):
        pl.semaphore_signal(barrier, inc=1, device_id={'ep': peer}, device_id_type=MESH)
    pl.semaphore_signal(barrier, inc=1, device_id={'rep': 1 - r}, device_id_type=MESH)

    @pl.when(z > 0)
    def _():
        pl.semaphore_signal(barrier, inc=1, device_id={'fsdp': (z + N_Z - 1) % N_Z}, device_id_type=MESH)

    @pl.when(z < N_Z - 1)
    def _():
        pl.semaphore_signal(barrier, inc=1, device_id={'fsdp': (z + 1) % N_Z}, device_id_type=MESH)

    own_w = [pltpu.make_async_copy(hbm[t].at[e], shard(t, e, z), own_sem.at[t, e])
             for e in range(n_local) for t in range(3)]
    own_x = pltpu.make_async_copy(x_hbm, toks.at[3], own_sem.at[3, 0])
    own_ids = pltpu.make_async_copy(ids_hbm, ids.at[3], own_sem.at[3, 1])
    own_gates = pltpu.make_async_copy(gates_hbm, gates.at[3], own_sem.at[3, 2])
    own_copies = own_w + [own_x, own_ids, own_gates]
    for copy in own_copies:
        copy.start()

    pl.semaphore_wait(barrier, 4 + (z + N_Z - 1) // N_Z + (2 * N_Z - 2 - z) // N_Z)

    meta = []
    for slot, peer in ((2, core_peer), (1, y_peer), (0, far_peer)):
        meta.append(remote(ids_hbm, ids.at[slot], meta_send.at[0, slot], meta_recv.at[0, slot], ep=peer))
        meta.append(remote(gates_hbm, gates.at[slot], meta_send.at[1, slot], meta_recv.at[1, slot], ep=peer))
    for copy in meta:
        copy.start()
    send_own(0)
    tok_core = remote(x_hbm, toks.at[2], tok_send.at[2], tok_recv.at[2], ep=core_peer)
    tok_y = remote(x_hbm, toks.at[1], tok_send.at[1], tok_recv.at[1], ep=y_peer)
    tok_far = remote(toks.at[1], toks.at[0], tok_send.at[0], tok_recv.at[0], ep=core_peer)
    tok_core.start()
    tok_y.start()

    def zero(i, carry):
        rows = pl.ds(pl.multiple_of(i % N_BLOCK * block, block), block)
        acc[i // N_BLOCK, rows, :] = jnp.zeros((block, acc.shape[2]), jnp.float32)
        return carry

    lax.fori_loop(0, 4 * N_BLOCK, zero, 0)

    for dist in range(1, N_Z):
        for t in range(3):
            event(0, dist, t)
    send_own(1)
    for copy in own_copies:
        copy.wait()
    tok_y.wait_recv()
    tok_far.start()
    for copy in meta:
        copy.wait_recv()
    tok_core.wait_recv()
    wait_x(0)
    tok_far.wait_recv()

    def compute(e, slot, row, block):
        rows = pl.ds(pl.multiple_of(row * block, block), block)
        x = toks[slot, rows, :]
        a = jnp.dot(x, wg[e], preferred_element_type=jnp.float32)
        b = jnp.dot(x, wu[e], preferred_element_type=jnp.float32)
        h = (a * jax.nn.sigmoid(a) * b).astype(jnp.bfloat16)
        o = jnp.dot(h, wd[e], preferred_element_type=jnp.float32).astype(jnp.bfloat16).astype(jnp.float32)
        expert = p * n_local + e
        chosen = jnp.where(ids[slot, :, rows] == expert, gates[slot, :, rows], 0.0)
        gate = jnp.sum(chosen, axis=0, keepdims=True)
        gate = jnp.broadcast_to(gate, (128, block)).T
        for c in range(acc.shape[2] // 128):
            cols = slice(c * 128, (c + 1) * 128)
            acc[slot, rows, cols] += jnp.where(gate > 0, gate * o[:, cols], 0.0)

    n_step = 4 * N_BLOCK * 2

    def packet(k, carry):
        def step(i, carry):
            for j in range(9):
                @pl.when(i == j * n_step // 9)
                def _():
                    event(k + 1, j // 3 + 1, j % 3)

            @pl.when((i == 8 * n_step // 9) & (k + 2 < n_packet))
            def _():
                send_own(k + 2)
            compute(2 * k + i % 2, i // 2 // N_BLOCK, i // 2 % N_BLOCK, block)
            return carry

        lax.fori_loop(0, n_step, step, 0)

        @pl.when(k + 2 < n_packet)
        def _():
            wait_x(k + 1)
        return carry

    lax.fori_loop(0, n_packet - 1, packet, 0)

    tail = n_tok // N_TAIL
    last = n_packet - 1

    def block_of(ref, row):
        return ref.at[pl.ds(row * tail, tail), :]

    def to_core(slot, row):
        return remote(block_of(acc.at[slot], row), block_of(from_core, row),
                      sum_send.at[slot, row], sum_recv.at[slot, row], ep=core_peer)

    def to_y(row):
        return remote(block_of(acc.at[1], row), block_of(from_y, row),
                      sum_send.at[1, row], sum_recv.at[1, row], ep=y_peer)

    def far_first(i, carry):
        compute(2 * last + r, i % 2, i // 2, block)
        return carry

    lax.fori_loop(0, 2 * N_BLOCK, far_first, 0)
    wait_x(last)

    def far_second(i, carry):
        compute(2 * last + 1 - r, i % 2, i // 2, tail)
        for n in range(N_TAIL):
            @pl.when(i == 2 * n)
            def _():
                to_core(0, n).start()

            @pl.when(i == 2 * n + 1)
            def _():
                to_core(0, n).wait_recv()
                rows = slice(n * tail, (n + 1) * tail)
                acc[1, rows, :] += from_core[rows, :]
                to_y(n).start()
                pl.semaphore_signal(credit.at[n], inc=1, device_id={'ep': core_peer}, device_id_type=MESH)
        return carry

    lax.fori_loop(0, 2 * N_TAIL, far_second, 0)

    def near(i, carry):
        compute(2 * last + i % 2, 2 + i // 2 // N_TAIL, i // 2 % N_TAIL, tail)
        for n in range(N_TAIL):
            @pl.when(i == 2 * n + 1)
            def _():
                pl.semaphore_wait(credit.at[n], 1)
                to_core(2, n).start()
        return carry

    lax.fori_loop(0, 4 * N_TAIL, near, 0)

    outs = []
    for n in range(N_TAIL):
        rows = slice(n * tail, (n + 1) * tail)
        to_core(2, n).wait_recv()
        acc[3, rows, :] += toks[3, rows, :].astype(jnp.float32) + from_core[rows, :]
    for n in range(N_TAIL):
        rows = slice(n * tail, (n + 1) * tail)
        to_y(n).wait_recv()
        toks[3, rows, :] = (acc[3, rows, :] + from_y[rows, :]).astype(jnp.bfloat16)
        copy = pltpu.make_async_copy(block_of(toks.at[3], n), block_of(out_hbm, n), out_sem.at[n])
        copy.start()
        outs.append(copy)

    for copy in meta + [tok_core, tok_y, tok_far]:
        copy.wait_send()
    for n in range(N_TAIL):
        to_core(0, n).wait_send()
        to_y(n).wait_send()
        to_core(2, n).wait_send()

    def drain(k, carry):
        for t in range(3):
            @pl.when(z > 0)
            def _():
                z_copy(t, k, z, False, True).wait_send()

            @pl.when(z < N_Z - 1)
            def _():
                z_copy(t, k, z, True, True).wait_send()
            for dist in range(1, N_Z):
                left = (z + N_Z - dist) % N_Z
                right = (z + dist) % N_Z

                @pl.when((z + dist < N_Z) & (z > 0))
                def _():
                    z_copy(t, k, right, False, False).wait_send()

                @pl.when((z >= dist) & (z < N_Z - 1))
                def _():
                    z_copy(t, k, left, True, False).wait_send()
                x_copy(t, k, (z + dist) % N_Z).wait_send()
        return carry

    lax.fori_loop(0, n_packet, drain, 0)
    for copy in outs:
        copy.wait()


def solution(mesh):
    tok_spec = P(('rep', 'fsdp', 'ep'), None)

    def device_step(x_blk, ids_blk, gate_blk, wg_blk, wu_blk, wd_blk):
        n_tok, d_model = x_blk.shape
        n_choice = ids_blk.shape[1]
        n_local, d_shard, ffn = wg_blk.shape
        dma = pltpu.SemaphoreType.DMA
        n_packet = n_local // 2
        any_space = pl.BlockSpec(memory_space=pl.ANY)
        flops = 4 * n_tok * n_local * 6 * d_model * ffn
        return pl.pallas_call(
            moe_kernel,
            out_shape=jax.ShapeDtypeStruct((n_tok, d_model), jnp.bfloat16),
            in_specs=[any_space] * 6,
            out_specs=any_space,
            scratch_shapes=[
                pltpu.VMEM((n_local, d_model, ffn), jnp.bfloat16),
                pltpu.VMEM((n_local, d_model, ffn), jnp.bfloat16),
                pltpu.VMEM((n_local, ffn, d_model), jnp.bfloat16),
                pltpu.VMEM((4, n_tok, d_model), jnp.bfloat16),
                pltpu.VMEM((4, n_choice, n_tok), jnp.int32),
                pltpu.VMEM((4, n_choice, n_tok), jnp.float32),
                pltpu.VMEM((4, n_tok, d_model), jnp.float32),
                pltpu.VMEM((n_tok, d_model), jnp.float32),
                pltpu.VMEM((n_tok, d_model), jnp.float32),
                dma((4, n_local)),
                dma((3, n_packet, N_Z)),
                dma((3, n_packet, N_Z)),
                dma((3, n_packet, N_Z)),
                dma((3, n_packet, N_Z)),
                dma((3, n_packet, N_Z)),
                dma((3,)),
                dma((3,)),
                dma((2, 3)),
                dma((2, 3)),
                dma((3, N_TAIL)),
                dma((3, N_TAIL)),
                pltpu.SemaphoreType.REGULAR((N_TAIL,)),
                dma((N_TAIL,)),
            ],
            compiler_params=pltpu.CompilerParams(
                collective_id=0, has_side_effects=True, vmem_limit_bytes=67043328),
            cost_estimate=pl.CostEstimate(flops=flops, bytes_accessed=32 << 20, transcendentals=0),
            name='moe',
        )(x_blk, ids_blk.T, gate_blk.T, wg_blk, wu_blk, wd_blk)

    return jax.shard_map(
        device_step, mesh=mesh,
        in_specs=(tok_spec, tok_spec, tok_spec, P('ep', 'fsdp', None), P('ep', 'fsdp', None), P('ep', None, 'fsdp')),
        out_specs=tok_spec, check_vma=False)
```

```python
import functools

import jax
import jax.numpy as jnp
from jax import lax
from jax.experimental import pallas as pl
from jax.experimental.pallas import tpu as pltpu
from jax.sharding import PartitionSpec as P

MESH = pl.DeviceIdType.MESH
N_Z = 4
N_BLOCK = 2
N_TAIL = 4


def moe_kernel(x_hbm, ids_hbm, gates_hbm, wg_hbm, wu_hbm, wd_hbm, out_hbm,
               wg, wu, wd, toks, ids, gates, acc, from_core, from_y,
               own_sem, recv_z, recv_x, send_r, send_l, send_x,
               tok_send, tok_recv, meta_send, meta_recv, home_send, home_recv, free,
               sum_send, sum_recv, credit, out_sem):
    r = lax.axis_index('rep')
    z = lax.axis_index('fsdp')
    p = lax.axis_index('ep')
    core = p % 2
    core_peer = p + 1 - 2 * core
    y_peer = (p + 2) % 4
    far_peer = (core_peer + 2) % 4
    n_local = wg_hbm.shape[0]
    n_packet = n_local // 2
    d_shard = wg_hbm.shape[1]
    n_tok = x_hbm.shape[0]
    block = n_tok // N_BLOCK

    hbm = (wg_hbm, wu_hbm, wd_hbm)

    def shard(t, e, s):
        start = pl.multiple_of(s * d_shard, d_shard)
        if t == 2:
            return wd.at[e, :, pl.ds(start, d_shard)]
        return (wg, wu)[t].at[e, pl.ds(start, d_shard), :]

    def remote(src, dst, send_sem, recv_sem, **where):
        return pltpu.make_async_remote_copy(src_ref=src, dst_ref=dst, send_sem=send_sem, recv_sem=recv_sem,
                                            device_id=where, device_id_type=MESH)

    def place(k):
        return 2 * (k % n_packet)

    def z_copy(t, k, s, right, own):
        e = place(k) + r
        src = hbm[t].at[e] if own else shard(t, e, s)
        send = send_r if right else send_l
        to = (z + 1) % N_Z if right else (z + N_Z - 1) % N_Z
        return remote(src, shard(t, e, s), send.at[t, k, s], recv_z.at[t, k, s], fsdp=to)

    def x_copy(t, k, s):
        e = place(k) + r
        return remote(shard(t, e, s), shard(t, e, s), send_x.at[t, k, s], recv_x.at[t, k, s], rep=1 - r)

    def x_arrival(t, k, s):
        e = place(k) + 1 - r
        return remote(shard(t, e, s), shard(t, e, s), send_x.at[t, k, s], recv_x.at[t, k, s], rep=1 - r)

    def home_copy(t, q):
        return remote(hbm[t].at[n_local - 2 + q], shard(t, q, z), home_send.at[t, q], home_recv.at[t, q], ep=y_peer)

    def send_own(k, t, own=True):
        @pl.when(z > 0)
        def _():
            z_copy(t, k, z, False, own).start()

        @pl.when(z < N_Z - 1)
        def _():
            z_copy(t, k, z, True, own).start()

    def signal_neighbours(sem, peers):
        for peer in peers:
            pl.semaphore_signal(sem, inc=1, device_id={'ep': peer}, device_id_type=MESH)
        pl.semaphore_signal(sem, inc=1, device_id={'rep': 1 - r}, device_id_type=MESH)

        @pl.when(z > 0)
        def _():
            pl.semaphore_signal(sem, inc=1, device_id={'fsdp': (z + N_Z - 1) % N_Z}, device_id_type=MESH)

        @pl.when(z < N_Z - 1)
        def _():
            pl.semaphore_signal(sem, inc=1, device_id={'fsdp': (z + 1) % N_Z}, device_id_type=MESH)

    def event(k, dist, t):
        left = (z + N_Z - dist) % N_Z
        right = (z + dist) % N_Z

        @pl.when(z + dist < N_Z)
        def _():
            z_copy(t, k, right, False, False).wait_recv()

            @pl.when(z > 0)
            def _():
                z_copy(t, k, right, False, False).start()
            x_copy(t, k, right).start()

        @pl.when(z >= dist)
        def _():
            z_copy(t, k, left, True, False).wait_recv()

            @pl.when(z < N_Z - 1)
            def _():
                z_copy(t, k, left, True, False).start()
            x_copy(t, k, left).start()

    def wait_x(k):
        for dist in range(1, N_Z):
            for t in range(3):
                x_arrival(t, k, (z + dist) % N_Z).wait_recv()

    barrier = pltpu.get_barrier_semaphore()
    signal_neighbours(barrier, (core_peer, y_peer, far_peer))

    own_w = [pltpu.make_async_copy(hbm[t].at[e], shard(t, e, z), own_sem.at[t, e])
             for e in range(n_local) for t in range(3)]
    own_x = pltpu.make_async_copy(x_hbm, toks.at[3], own_sem.at[3, 0])
    own_ids = pltpu.make_async_copy(ids_hbm, ids.at[3], own_sem.at[3, 1])
    own_gates = pltpu.make_async_copy(gates_hbm, gates.at[3], own_sem.at[3, 2])
    own_copies = own_w + [own_x, own_ids, own_gates]
    for copy in own_copies:
        copy.start()

    z_peers = (z + N_Z - 1) // N_Z + (2 * N_Z - 2 - z) // N_Z
    pl.semaphore_wait(barrier, 4 + z_peers)

    meta = []
    for slot, peer in ((2, core_peer), (1, y_peer), (0, far_peer)):
        meta.append(remote(ids_hbm, ids.at[slot], meta_send.at[0, slot], meta_recv.at[0, slot], ep=peer))
        meta.append(remote(gates_hbm, gates.at[slot], meta_send.at[1, slot], meta_recv.at[1, slot], ep=peer))
    for copy in meta:
        copy.start()
    for t in range(3):
        send_own(0, t)
    tok_core = remote(x_hbm, toks.at[2], tok_send.at[2], tok_recv.at[2], ep=core_peer)
    tok_y = remote(x_hbm, toks.at[1], tok_send.at[1], tok_recv.at[1], ep=y_peer)
    tok_far = remote(toks.at[1], toks.at[0], tok_send.at[0], tok_recv.at[0], ep=core_peer)
    tok_core.start()
    tok_y.start()

    def zero(i, carry):
        rows = pl.ds(pl.multiple_of(i % N_BLOCK * block, block), block)
        acc[i // N_BLOCK, rows, :] = jnp.zeros((block, acc.shape[2]), jnp.float32)
        return carry

    lax.fori_loop(0, 4 * N_BLOCK, zero, 0)

    for dist in range(1, N_Z):
        for t in range(3):
            event(0, dist, t)
            if dist == 3:
                send_own(1, t)
    for copy in own_copies:
        copy.wait()
    tok_y.wait_recv()
    tok_far.start()
    for copy in meta:
        copy.wait_recv()
    tok_core.wait_recv()
    wait_x(0)
    tok_far.wait_recv()

    def compute(e, slot, row, block, group=None):
        rows = pl.ds(pl.multiple_of(row * block, block), block)
        x = toks[slot, rows, :]
        a = jnp.dot(x, wg[e], preferred_element_type=jnp.float32)
        b = jnp.dot(x, wu[e], preferred_element_type=jnp.float32)
        h = (a * jax.nn.sigmoid(a) * b).astype(jnp.bfloat16)
        o = jnp.dot(h, wd[e], preferred_element_type=jnp.float32).astype(jnp.bfloat16).astype(jnp.float32)
        expert = p * n_local + e if group is None else group * n_local + n_local - 2 + e
        chosen = jnp.where(ids[slot, :, rows] == expert, gates[slot, :, rows], 0.0)
        gate = jnp.sum(chosen, axis=0, keepdims=True)
        gate = jnp.broadcast_to(gate, (128, block)).T
        for c in range(acc.shape[2] // 128):
            cols = slice(c * 128, (c + 1) * 128)
            acc[slot, rows, cols] += jnp.where(gate > 0, gate * o[:, cols], 0.0)

    def drain(k, own=True):
        for t in range(3):
            @pl.when(z > 0)
            def _():
                z_copy(t, k, z, False, own).wait_send()

            @pl.when(z < N_Z - 1)
            def _():
                z_copy(t, k, z, True, own).wait_send()
            for dist in range(1, N_Z):
                left = (z + N_Z - dist) % N_Z
                right = (z + dist) % N_Z

                @pl.when((z + dist < N_Z) & (z > 0))
                def _():
                    z_copy(t, k, right, False, False).wait_send()

                @pl.when((z >= dist) & (z < N_Z - 1))
                def _():
                    z_copy(t, k, left, True, False).wait_send()
                x_copy(t, k, (z + dist) % N_Z).wait_send()

    def events(i, k, first, steps):
        for n, at in enumerate(steps):
            j = first + n

            @pl.when(i == at)
            def _():
                event(k, j // 3 + 1, j % 3)

    n_step = 4 * N_BLOCK * 2
    last = n_packet - 1
    spread = [j * n_step // 9 for j in range(9)]

    def packet(k, carry):
        def step(i, carry):
            for j in range(9):
                @pl.when(i == spread[j])
                def _():
                    event(k + 1, j // 3 + 1, j % 3)
                    if j >= 6:
                        send_own(k + 2, j - 6)

            @pl.when((k == 1) & (i == 2))
            def _():
                pl.semaphore_wait(free, 2 + z_peers)
                for q in range(2):
                    for t in range(3):
                        home_copy(t, q).start()
            compute(2 * k + i % 2, i // 2 // N_BLOCK, i // 2 % N_BLOCK, block)
            return carry

        lax.fori_loop(0, n_step, step, 0)

        @pl.when(k == 0)
        def _():
            wait_x(1)
            drain(0)
            signal_neighbours(free, (y_peer,))
        return carry

    lax.fori_loop(0, last - 1, packet, 0)

    tail = n_tok // N_TAIL

    def block_of(ref, row):
        return ref.at[pl.ds(row * tail, tail), :]

    def to_core(slot, row):
        return remote(block_of(acc.at[slot], row), block_of(from_core, row),
                      sum_send.at[slot, row], sum_recv.at[slot, row], ep=core_peer)

    def to_y(row):
        return remote(block_of(acc.at[1], row), block_of(from_y, row),
                      sum_send.at[1, row], sum_recv.at[1, row], ep=y_peer)

    def far_first(i, carry):
        events(i, last, 0, (0, 2))
        compute(2 * last - 2 + r, i % 2, i // 2, block)
        return carry

    lax.fori_loop(0, 2 * N_BLOCK, far_first, 0)
    wait_x(last - 1)

    def far_second(i, carry):
        events(i, last, 2, (1, 4, 7))
        compute(2 * last - 1 - r, i % 2, i // 2, tail)
        for n in range(N_TAIL):
            @pl.when(i == 2 * n)
            def _():
                to_core(0, n).start()

            @pl.when(i == 2 * n + 1)
            def _():
                to_core(0, n).wait_recv()
                rows = slice(n * tail, (n + 1) * tail)
                acc[1, rows, :] += from_core[rows, :]
                to_y(n).start()
                pl.semaphore_signal(credit.at[n], inc=1, device_id={'ep': core_peer}, device_id_type=MESH)
        return carry

    lax.fori_loop(0, 2 * N_TAIL, far_second, 0)

    def near(i, carry):
        events(i, last, 5, (1, 2, 4, 6))
        for t, at in enumerate((2, 4, 6)):
            @pl.when(i == at)
            def _():
                for q in range(2):
                    home_copy(t, q).wait_recv()
                send_own(n_packet, t, False)
        compute(2 * last - 2 + i % 2, 2 + i // 2 // N_BLOCK, i // 2 % N_BLOCK, block)
        return carry

    lax.fori_loop(0, 4 * N_BLOCK, near, 0)
    wait_x(last)

    def home(i, carry):
        events(i, n_packet, 0, [j * 4 * N_BLOCK // 9 for j in range(9)])
        compute(2 * last + i % 2, 2 + i // 2 // N_BLOCK, i // 2 % N_BLOCK, block)
        return carry

    lax.fori_loop(0, 4 * N_BLOCK, home, 0)

    def peer_first(i, carry):
        compute(r, 2 + i // N_BLOCK, i % N_BLOCK, block, y_peer)
        return carry

    lax.fori_loop(0, 2 * N_BLOCK, peer_first, 0)
    wait_x(n_packet)

    def peer_second(i, carry):
        compute(1 - r, 2 + i // N_TAIL, i % N_TAIL, tail, y_peer)
        for n in range(N_TAIL):
            @pl.when(i == n)
            def _():
                pl.semaphore_wait(credit.at[n], 1)
                to_core(2, n).start()
        return carry

    lax.fori_loop(0, 2 * N_TAIL, peer_second, 0)

    outs = []
    for n in range(N_TAIL):
        rows = slice(n * tail, (n + 1) * tail)
        to_core(2, n).wait_recv()
        acc[3, rows, :] += toks[3, rows, :].astype(jnp.float32) + from_core[rows, :]
    for n in range(N_TAIL):
        rows = slice(n * tail, (n + 1) * tail)
        to_y(n).wait_recv()
        toks[3, rows, :] = (acc[3, rows, :] + from_y[rows, :]).astype(jnp.bfloat16)
        copy = pltpu.make_async_copy(block_of(toks.at[3], n), block_of(out_hbm, n), out_sem.at[n])
        copy.start()
        outs.append(copy)

    for copy in meta + [tok_core, tok_y, tok_far]:
        copy.wait_send()
    for n in range(N_TAIL):
        to_core(0, n).wait_send()
        to_y(n).wait_send()
        to_core(2, n).wait_send()

    for t in range(3):
        for q in range(2):
            home_copy(t, q).wait_send()

    def drain_step(k, carry):
        drain(k)
        return carry

    lax.fori_loop(1, n_packet, drain_step, 0)
    drain(n_packet, False)
    for copy in outs:
        copy.wait()


def solution(mesh):
    tok_spec = P(('rep', 'fsdp', 'ep'), None)

    def device_step(x_blk, ids_blk, gate_blk, wg_blk, wu_blk, wd_blk):
        n_tok, d_model = x_blk.shape
        n_choice = ids_blk.shape[1]
        n_local, d_shard, ffn = wg_blk.shape
        dma = pltpu.SemaphoreType.DMA
        n_packet = n_local // 2
        any_space = pl.BlockSpec(memory_space=pl.ANY)
        flops = 4 * n_tok * n_local * 6 * d_model * ffn
        return pl.pallas_call(
            moe_kernel,
            out_shape=jax.ShapeDtypeStruct((n_tok, d_model), jnp.bfloat16),
            in_specs=[any_space] * 6,
            out_specs=any_space,
            scratch_shapes=[
                pltpu.VMEM((n_local, d_model, ffn), jnp.bfloat16),
                pltpu.VMEM((n_local, d_model, ffn), jnp.bfloat16),
                pltpu.VMEM((n_local, ffn, d_model), jnp.bfloat16),
                pltpu.VMEM((4, n_tok, d_model), jnp.bfloat16),
                pltpu.VMEM((4, n_choice, n_tok), jnp.int32),
                pltpu.VMEM((4, n_choice, n_tok), jnp.float32),
                pltpu.VMEM((4, n_tok, d_model), jnp.float32),
                pltpu.VMEM((n_tok, d_model), jnp.float32),
                pltpu.VMEM((n_tok, d_model), jnp.float32),
                dma((4, n_local)),
                dma((3, n_packet + 1, N_Z)),
                dma((3, n_packet + 1, N_Z)),
                dma((3, n_packet + 1, N_Z)),
                dma((3, n_packet + 1, N_Z)),
                dma((3, n_packet + 1, N_Z)),
                dma((3,)),
                dma((3,)),
                dma((2, 3)),
                dma((2, 3)),
                dma((3, 2)),
                dma((3, 2)),
                pltpu.SemaphoreType.REGULAR,
                dma((3, N_TAIL)),
                dma((3, N_TAIL)),
                pltpu.SemaphoreType.REGULAR((N_TAIL,)),
                dma((N_TAIL,)),
            ],
            compiler_params=pltpu.CompilerParams(
                collective_id=0, has_side_effects=True, vmem_limit_bytes=67043328),
            cost_estimate=pl.CostEstimate(flops=flops, bytes_accessed=32 << 20, transcendentals=0),
            name='moe',
        )(x_blk, ids_blk.T, gate_blk.T, wg_blk, wu_blk, wd_blk)

    return jax.shard_map(
        device_step, mesh=mesh,
        in_specs=(tok_spec, tok_spec, tok_spec, P('ep', 'fsdp', None), P('ep', 'fsdp', None), P('ep', None, 'fsdp')),
        out_specs=tok_spec, check_vma=False)
```

```python
import functools

import jax
import jax.numpy as jnp
from jax import lax
from jax.experimental import pallas as pl
from jax.experimental.pallas import tpu as pltpu
from jax.sharding import PartitionSpec as P

MESH = pl.DeviceIdType.MESH
N_Z = 4
N_BLOCK = 2
N_TAIL = 4
N_EVENT = 9
LEAD = 2
STEP_OF = (0, 0, 3, 4, 6, 9, 12, 13, 15)
STEP_OF_LAST = (2, 5, 6, 6, 8, 11, 12, 15, 17)
STEP_OF_PEER = (0, 0, 1, 3, 5, 8, 10, 13, 14)
OWN_AFTER = (5, 6, 7)
PEER_OWN_AFTER = (6, 10, 13)


def moe_kernel(x_hbm, ids_hbm, gates_hbm, wg_hbm, wu_hbm, wd_hbm, out_hbm,
               wg, wu, wd, toks, ids, gates, acc, from_core, from_y,
               own_sem, recv_z, recv_x, send_r, send_l, send_x,
               tok_send, tok_recv, meta_send, meta_recv, home_send, home_recv, free,
               sum_send, sum_recv, credit, out_sem):
    r = lax.axis_index('rep')
    z = lax.axis_index('fsdp')
    p = lax.axis_index('ep')
    core = p % 2
    core_peer = p + 1 - 2 * core
    y_peer = (p + 2) % 4
    far_peer = (core_peer + 2) % 4
    n_local = wg_hbm.shape[0]
    n_packet = n_local // 2
    d_shard = wg_hbm.shape[1]
    n_tok = x_hbm.shape[0]
    block = n_tok // N_BLOCK

    hbm = (wg_hbm, wu_hbm, wd_hbm)

    def shard(t, e, s):
        start = pl.multiple_of(s * d_shard, d_shard)
        if t == 2:
            return wd.at[e, :, pl.ds(start, d_shard)]
        return (wg, wu)[t].at[e, pl.ds(start, d_shard), :]

    def remote(src, dst, send_sem, recv_sem, **where):
        return pltpu.make_async_remote_copy(src_ref=src, dst_ref=dst, send_sem=send_sem, recv_sem=recv_sem,
                                            device_id=where, device_id_type=MESH)

    def place(k):
        return 2 * (k % n_packet)

    def z_copy(t, k, s, right, own):
        e = place(k) + r
        src = hbm[t].at[e] if own else shard(t, e, s)
        send = send_r if right else send_l
        to = (z + 1) % N_Z if right else (z + N_Z - 1) % N_Z
        return remote(src, shard(t, e, s), send.at[t, k, s], recv_z.at[t, k, s], fsdp=to)

    def x_copy(t, k, s):
        e = place(k) + r
        return remote(shard(t, e, s), shard(t, e, s), send_x.at[t, k, s], recv_x.at[t, k, s], rep=1 - r)

    def x_arrival(t, k, s):
        e = place(k) + 1 - r
        return remote(shard(t, e, s), shard(t, e, s), send_x.at[t, k, s], recv_x.at[t, k, s], rep=1 - r)

    def home_copy(t, q):
        return remote(hbm[t].at[n_local - 2 + q], shard(t, q, z), home_send.at[t, q], home_recv.at[t, q], ep=y_peer)

    def send_own(k, t, own=True):
        @pl.when(z > 0)
        def _():
            z_copy(t, k, z, False, own).start()

        @pl.when(z < N_Z - 1)
        def _():
            z_copy(t, k, z, True, own).start()

    def signal_neighbours(sem, peers):
        for peer in peers:
            pl.semaphore_signal(sem, inc=1, device_id={'ep': peer}, device_id_type=MESH)
        pl.semaphore_signal(sem, inc=1, device_id={'rep': 1 - r}, device_id_type=MESH)

        @pl.when(z > 0)
        def _():
            pl.semaphore_signal(sem, inc=1, device_id={'fsdp': (z + N_Z - 1) % N_Z}, device_id_type=MESH)

        @pl.when(z < N_Z - 1)
        def _():
            pl.semaphore_signal(sem, inc=1, device_id={'fsdp': (z + 1) % N_Z}, device_id_type=MESH)

    def event(k, j):
        peer_packet = isinstance(k, int) and k == n_packet
        dist, t = (j % 3 + 1, j // 3) if peer_packet else (j // 3 + 1, j % 3)
        left = (z + N_Z - dist) % N_Z
        right = (z + dist) % N_Z

        @pl.when(z + dist < N_Z)
        def _():
            z_copy(t, k, right, False, False).wait_recv()

            @pl.when(z > 0)
            def _():
                z_copy(t, k, right, False, False).start()
            x_copy(t, k, right).start()

        @pl.when(z >= dist)
        def _():
            z_copy(t, k, left, True, False).wait_recv()

            @pl.when(z < N_Z - 1)
            def _():
                z_copy(t, k, left, True, False).start()
            x_copy(t, k, left).start()

        last_packets = isinstance(k, int) and k >= n_packet - 1
        for t in range(3):
            if not last_packets and OWN_AFTER[t] == j:
                send_own(k + 1, t)
            if last_packets and PEER_OWN_AFTER[t] == (k - n_packet + 1) * N_EVENT + j:
                for q in range(2):
                    home_copy(t, q).wait_recv()
                send_own(n_packet, t, False)

    def wait_x(k, tensors=(0, 1, 2)):
        for dist in range(1, N_Z):
            for t in tensors:
                x_arrival(t, k, (z + dist) % N_Z).wait_recv()

    barrier = pltpu.get_barrier_semaphore()
    signal_neighbours(barrier, (core_peer, y_peer, far_peer))

    own_w = [pltpu.make_async_copy(hbm[t].at[e], shard(t, e, z), own_sem.at[t, e])
             for e in range(n_local) for t in range(3)]
    own_x = pltpu.make_async_copy(x_hbm, toks.at[3], own_sem.at[3, 0])
    own_ids = pltpu.make_async_copy(ids_hbm, ids.at[3], own_sem.at[3, 1])
    own_gates = pltpu.make_async_copy(gates_hbm, gates.at[3], own_sem.at[3, 2])
    own_copies = own_w + [own_x, own_ids, own_gates]
    for copy in own_copies:
        copy.start()

    z_peers = (z + N_Z - 1) // N_Z + (2 * N_Z - 2 - z) // N_Z
    pl.semaphore_wait(barrier, 4 + z_peers)

    meta = []
    for slot, peer in ((2, core_peer), (1, y_peer), (0, far_peer)):
        meta.append(remote(ids_hbm, ids.at[slot], meta_send.at[0, slot], meta_recv.at[0, slot], ep=peer))
        meta.append(remote(gates_hbm, gates.at[slot], meta_send.at[1, slot], meta_recv.at[1, slot], ep=peer))
    for copy in meta:
        copy.start()
    for t in range(3):
        send_own(0, t)
    tok_core = remote(x_hbm, toks.at[2], tok_send.at[2], tok_recv.at[2], ep=core_peer)
    tok_y = remote(x_hbm, toks.at[1], tok_send.at[1], tok_recv.at[1], ep=y_peer)
    tok_far = remote(toks.at[1], toks.at[0], tok_send.at[0], tok_recv.at[0], ep=core_peer)
    tok_core.start()
    tok_y.start()

    def zero(i, carry):
        rows = pl.ds(pl.multiple_of(i % N_BLOCK * block, block), block)
        acc[i // N_BLOCK, rows, :] = jnp.zeros((block, acc.shape[2]), jnp.float32)
        return carry

    lax.fori_loop(0, 4 * N_BLOCK, zero, 0)

    for j in range(N_EVENT):
        event(0, j)
    for copy in own_copies:
        copy.wait()
    tok_y.wait_recv()
    tok_far.start()
    for copy in meta:
        copy.wait_recv()
    tok_core.wait_recv()
    for j in range(LEAD):
        event(1, j)
    wait_x(0)
    tok_far.wait_recv()

    def hidden(e, slot, rows):
        x = toks[slot, rows, :]
        a = jnp.dot(x, wg[e], preferred_element_type=jnp.float32)
        b = jnp.dot(x, wu[e], preferred_element_type=jnp.float32)
        return (a * jax.nn.sigmoid(a) * b).astype(jnp.bfloat16)

    def add_output(h, w_down, expert, slot, rows, start, width):
        o = jnp.dot(h, w_down, preferred_element_type=jnp.float32).astype(jnp.bfloat16).astype(jnp.float32)
        chosen = jnp.where(ids[slot, :, rows] == expert, gates[slot, :, rows], 0.0)
        gate = jnp.sum(chosen, axis=0, keepdims=True)
        gate = jnp.broadcast_to(gate, (128, h.shape[0])).T
        for c in range(width // 128):
            cols = pl.ds(start + c * 128, 128)
            acc[slot, rows, cols] += jnp.where(gate > 0, gate * o[:, c * 128:(c + 1) * 128], 0.0)

    def rows_of(row, block):
        return pl.ds(pl.multiple_of(row * block, block), block)

    def compute(e, slot, row, block):
        rows = rows_of(row, block)
        add_output(hidden(e, slot, rows), wd[e], p * n_local + e, slot, rows, 0, acc.shape[2])

    ffn = wg.shape[2]

    def peer_hidden(e, slot, row):
        rows = rows_of(row, block)
        toks[slot - 2, rows, pl.ds(pl.multiple_of(e * ffn, ffn), ffn)] = hidden(e, slot, rows)

    def peer_output(e, slot, row, s):
        rows = rows_of(row, block)
        start = pl.multiple_of(s * d_shard, d_shard)
        h = toks[slot - 2, rows, pl.ds(pl.multiple_of(e * ffn, ffn), ffn)]
        expert = y_peer * n_local + n_local - 2 + e
        add_output(h, wd[e, :, pl.ds(start, d_shard)], expert, slot, rows, start, d_shard)

    def drain(k, own=True):
        for t in range(3):
            @pl.when(z > 0)
            def _():
                z_copy(t, k, z, False, own).wait_send()

            @pl.when(z < N_Z - 1)
            def _():
                z_copy(t, k, z, True, own).wait_send()
            for dist in range(1, N_Z):
                left = (z + N_Z - dist) % N_Z
                right = (z + dist) % N_Z

                @pl.when((z + dist < N_Z) & (z > 0))
                def _():
                    z_copy(t, k, right, False, False).wait_send()

                @pl.when((z >= dist) & (z < N_Z - 1))
                def _():
                    z_copy(t, k, left, True, False).wait_send()
                x_copy(t, k, (z + dist) % N_Z).wait_send()

    def events(i, k, steps, first=0, offset=0):
        for j in range(first, N_EVENT):
            if steps[j] >= offset:
                @pl.when(i == steps[j] - offset)
                def _():
                    event(k, j)

    n_step = 4 * N_BLOCK * 2
    last = n_packet - 1

    def packet(k, carry):
        def step(i, carry):
            events(i, k + 1, STEP_OF, LEAD)

            @pl.when((k == 1) & (i == 2))
            def _():
                pl.semaphore_wait(free, 2 + z_peers)
                for t in range(3):
                    for q in range(2):
                        home_copy(t, q).start()
            compute(2 * k + i % 2, i // 2 // N_BLOCK, i // 2 % N_BLOCK, block)
            return carry

        lax.fori_loop(0, n_step, step, 0)

        @pl.when(k == 0)
        def _():
            for j in range(LEAD):
                event(2, j)
            wait_x(1)
            drain(0)
            signal_neighbours(free, (y_peer,))
        return carry

    lax.fori_loop(0, last - 1, packet, 0)

    tail = n_tok // N_TAIL

    def block_of(ref, row):
        return ref.at[pl.ds(row * tail, tail), :]

    def to_core(row):
        return remote(block_of(acc.at[0], row), block_of(from_core, row),
                      sum_send.at[0, row], sum_recv.at[0, row], ep=core_peer)

    def shard_at(n):
        return (z + n + z // 2 * (N_Z - 2 * n)) % N_Z

    def columns(n):
        return pl.ds(pl.multiple_of(shard_at(n) * d_shard, d_shard), d_shard)

    def to_core_near(n):
        return remote(acc.at[2, :, columns(n)], from_core.at[:, columns(n)],
                      sum_send.at[2, n], sum_recv.at[2, n], ep=core_peer)

    def to_y(row):
        return remote(block_of(acc.at[1], row), block_of(from_y, row),
                      sum_send.at[1, row], sum_recv.at[1, row], ep=y_peer)

    def far_first(i, carry):
        events(i, last, STEP_OF_LAST)
        compute(2 * last - 2 + r, i % 2, i // 2, block)
        return carry

    lax.fori_loop(0, 2 * N_BLOCK, far_first, 0)
    wait_x(last - 1)

    def far_second(i, carry):
        events(i, last, STEP_OF_LAST, offset=2 * N_BLOCK)
        compute(2 * last - 1 - r, i % 2, i // 2, tail)
        for n in range(N_TAIL):
            @pl.when(i == 2 * n)
            def _():
                to_core(n).start()

            @pl.when(i == 2 * n + 1)
            def _():
                to_core(n).wait_recv()
                rows = slice(n * tail, (n + 1) * tail)
                acc[1, rows, :] += from_core[rows, :]
                to_y(n).start()
                pl.semaphore_signal(credit.at[n], inc=1, device_id={'ep': core_peer}, device_id_type=MESH)
        return carry

    lax.fori_loop(0, 2 * N_TAIL, far_second, 0)

    def near(i, carry):
        events(i, last, STEP_OF_LAST, offset=2 * N_BLOCK + 2 * N_TAIL)
        compute(2 * last - 2 + i % 2, 2 + i // 2 // N_BLOCK, i // 2 % N_BLOCK, block)
        return carry

    lax.fori_loop(0, 4 * N_BLOCK, near, 0)
    for j in range(LEAD):
        event(n_packet, j)
    wait_x(last)

    def home(i, carry):
        events(i, n_packet, STEP_OF_PEER, LEAD)
        compute(2 * last + i % 2, 2 + i // 2 // N_BLOCK, i // 2 % N_BLOCK, block)
        return carry

    lax.fori_loop(0, 4 * N_BLOCK, home, 0)
    tok_far.wait_send()

    def peer_first(i, carry):
        events(i, n_packet, STEP_OF_PEER, LEAD, offset=4 * N_BLOCK)
        peer_hidden(r, 2 + i // N_BLOCK, i % N_BLOCK)
        return carry

    lax.fori_loop(0, 2 * N_BLOCK, peer_first, 0)
    wait_x(n_packet, (0, 1))

    def peer_second(i, carry):
        events(i, n_packet, STEP_OF_PEER, LEAD, offset=6 * N_BLOCK)
        peer_hidden(1 - r, 2 + i // N_BLOCK, i % N_BLOCK)
        return carry

    lax.fori_loop(0, 2 * N_BLOCK, peer_second, 0)
    for n in range(N_TAIL):
        pl.semaphore_wait(credit.at[n], 1)

    for n in range(N_Z):
        s = shard_at(n)
        if n > 0:
            x_arrival(2, n_packet, s).wait_recv()
        for slot in (2, 3):
            def output(i, carry):
                peer_output(i % 2, slot, i // 2, s)
                return carry

            lax.fori_loop(0, 2 * N_BLOCK, output, 0)
            if slot == 2:
                to_core_near(n).start()

    for n in range(N_TAIL):
        to_y(n).wait_recv()
    outs = []
    for n in range(N_Z):
        to_core_near(n).wait_recv()
        cols = columns(n)
        y = toks[3, :, cols].astype(jnp.float32) + (acc[3, :, cols] + from_core[:, cols] + from_y[:, cols])
        toks[3, :, cols] = y.astype(jnp.bfloat16)
        copy = pltpu.make_async_copy(toks.at[3, :, cols], out_hbm.at[:, cols], out_sem.at[n])
        copy.start()
        outs.append(copy)

    for copy in meta + [tok_core, tok_y]:
        copy.wait_send()
    for n in range(N_TAIL):
        to_core(n).wait_send()
        to_y(n).wait_send()
        to_core_near(n).wait_send()

    for t in range(3):
        for q in range(2):
            home_copy(t, q).wait_send()

    def drain_step(k, carry):
        drain(k)
        return carry

    lax.fori_loop(1, n_packet, drain_step, 0)
    drain(n_packet, False)
    for copy in outs:
        copy.wait()


def solution(mesh):
    tok_spec = P(('rep', 'fsdp', 'ep'), None)

    def device_step(x_blk, ids_blk, gate_blk, wg_blk, wu_blk, wd_blk):
        n_tok, d_model = x_blk.shape
        n_choice = ids_blk.shape[1]
        n_local, d_shard, ffn = wg_blk.shape
        dma = pltpu.SemaphoreType.DMA
        n_packet = n_local // 2
        any_space = pl.BlockSpec(memory_space=pl.ANY)
        flops = 4 * n_tok * n_local * 6 * d_model * ffn
        return pl.pallas_call(
            moe_kernel,
            out_shape=jax.ShapeDtypeStruct((n_tok, d_model), jnp.bfloat16),
            in_specs=[any_space] * 6,
            out_specs=any_space,
            scratch_shapes=[
                pltpu.VMEM((n_local, d_model, ffn), jnp.bfloat16),
                pltpu.VMEM((n_local, d_model, ffn), jnp.bfloat16),
                pltpu.VMEM((n_local, ffn, d_model), jnp.bfloat16),
                pltpu.VMEM((4, n_tok, d_model), jnp.bfloat16),
                pltpu.VMEM((4, n_choice, n_tok), jnp.int32),
                pltpu.VMEM((4, n_choice, n_tok), jnp.float32),
                pltpu.VMEM((4, n_tok, d_model), jnp.float32),
                pltpu.VMEM((n_tok, d_model), jnp.float32),
                pltpu.VMEM((n_tok, d_model), jnp.float32),
                dma((4, n_local)),
                dma((3, n_packet + 1, N_Z)),
                dma((3, n_packet + 1, N_Z)),
                dma((3, n_packet + 1, N_Z)),
                dma((3, n_packet + 1, N_Z)),
                dma((3, n_packet + 1, N_Z)),
                dma((3,)),
                dma((3,)),
                dma((2, 3)),
                dma((2, 3)),
                dma((3, 2)),
                dma((3, 2)),
                pltpu.SemaphoreType.REGULAR,
                dma((3, N_TAIL)),
                dma((3, N_TAIL)),
                pltpu.SemaphoreType.REGULAR((N_TAIL,)),
                dma((N_TAIL,)),
            ],
            compiler_params=pltpu.CompilerParams(
                collective_id=0, has_side_effects=True, vmem_limit_bytes=67043328),
            cost_estimate=pl.CostEstimate(flops=flops, bytes_accessed=32 << 20, transcendentals=0),
            name='moe',
        )(x_blk, ids_blk.T, gate_blk.T, wg_blk, wu_blk, wd_blk)

    return jax.shard_map(
        device_step, mesh=mesh,
        in_specs=(tok_spec, tok_spec, tok_spec, P('ep', 'fsdp', None), P('ep', 'fsdp', None), P('ep', None, 'fsdp')),
        out_specs=tok_spec, check_vma=False)
```

```python
import functools

import jax
import jax.numpy as jnp
from jax import lax
from jax.experimental import pallas as pl
from jax.experimental.pallas import tpu as pltpu
from jax.sharding import PartitionSpec as P

MESH = pl.DeviceIdType.MESH
N_Z = 4
N_BLOCK = 2
N_TAIL = 4
N_EVENT = 9
LEAD = 2
STEP_OF = (0, 0, 3, 4, 6, 9, 12, 13, 15)
STEP_OF_LAST = (2, 5, 6, 6, 8, 11, 12, 15, 17)
STEP_OF_PEER = (0, 0, 1, 3, 5, 8, 10, 14, 16)
OWN_AFTER = (5, 6, 7)
PEER_OWN_AFTER = (6, 10, 13)


def moe_kernel(x_hbm, ids_hbm, gates_hbm, wg_hbm, wu_hbm, wd_hbm, out_hbm,
               wg, wu, wd, toks, ids, gates, acc, from_core, from_y,
               own_sem, recv_z, recv_x, send_r, send_l, send_x,
               tok_send, tok_recv, meta_send, meta_recv, home_send, home_recv, free,
               sum_send, sum_recv, credit, out_sem):
    r = lax.axis_index('rep')
    z = lax.axis_index('fsdp')
    p = lax.axis_index('ep')
    core = p % 2
    core_peer = p + 1 - 2 * core
    y_peer = (p + 2) % 4
    far_peer = (core_peer + 2) % 4
    n_local = wg_hbm.shape[0]
    n_packet = n_local // 2
    d_shard = wg_hbm.shape[1]
    n_tok = x_hbm.shape[0]
    block = n_tok // N_BLOCK

    hbm = (wg_hbm, wu_hbm, wd_hbm)

    def shard(t, e, s):
        start = pl.multiple_of(s * d_shard, d_shard)
        if t == 2:
            return wd.at[e, :, pl.ds(start, d_shard)]
        return (wg, wu)[t].at[e, pl.ds(start, d_shard), :]

    def remote(src, dst, send_sem, recv_sem, **where):
        return pltpu.make_async_remote_copy(src_ref=src, dst_ref=dst, send_sem=send_sem, recv_sem=recv_sem,
                                            device_id=where, device_id_type=MESH)

    def place(k):
        return 2 * (k % n_packet)

    def z_copy(t, k, s, right, own):
        e = place(k) + r
        src = hbm[t].at[e] if own else shard(t, e, s)
        send = send_r if right else send_l
        to = (z + 1) % N_Z if right else (z + N_Z - 1) % N_Z
        return remote(src, shard(t, e, s), send.at[t, k, s], recv_z.at[t, k, s], fsdp=to)

    def x_copy(t, k, s):
        e = place(k) + r
        return remote(shard(t, e, s), shard(t, e, s), send_x.at[t, k, s], recv_x.at[t, k, s], rep=1 - r)

    def x_arrival(t, k, s):
        e = place(k) + 1 - r
        return remote(shard(t, e, s), shard(t, e, s), send_x.at[t, k, s], recv_x.at[t, k, s], rep=1 - r)

    def home_copy(t, q):
        return remote(hbm[t].at[n_local - 2 + q], shard(t, q, z), home_send.at[t, q], home_recv.at[t, q], ep=y_peer)

    def send_own(k, t, own=True):
        @pl.when(z > 0)
        def _():
            z_copy(t, k, z, False, own).start()

        @pl.when(z < N_Z - 1)
        def _():
            z_copy(t, k, z, True, own).start()

    def signal_neighbours(sem, peers):
        for peer in peers:
            pl.semaphore_signal(sem, inc=1, device_id={'ep': peer}, device_id_type=MESH)
        pl.semaphore_signal(sem, inc=1, device_id={'rep': 1 - r}, device_id_type=MESH)

        @pl.when(z > 0)
        def _():
            pl.semaphore_signal(sem, inc=1, device_id={'fsdp': (z + N_Z - 1) % N_Z}, device_id_type=MESH)

        @pl.when(z < N_Z - 1)
        def _():
            pl.semaphore_signal(sem, inc=1, device_id={'fsdp': (z + 1) % N_Z}, device_id_type=MESH)

    def event(k, j):
        peer_packet = isinstance(k, int) and k == n_packet
        dist, t = (j % 3 + 1, j // 3) if peer_packet else (j // 3 + 1, j % 3)
        left = (z + N_Z - dist) % N_Z
        right = (z + dist) % N_Z

        @pl.when(z + dist < N_Z)
        def _():
            z_copy(t, k, right, False, False).wait_recv()

            @pl.when(z > 0)
            def _():
                z_copy(t, k, right, False, False).start()
            x_copy(t, k, right).start()

        @pl.when(z >= dist)
        def _():
            z_copy(t, k, left, True, False).wait_recv()

            @pl.when(z < N_Z - 1)
            def _():
                z_copy(t, k, left, True, False).start()
            x_copy(t, k, left).start()

        last_packets = isinstance(k, int) and k >= n_packet - 1
        for t in range(3):
            if not last_packets and OWN_AFTER[t] == j:
                send_own(k + 1, t)
            if last_packets and PEER_OWN_AFTER[t] == (k - n_packet + 1) * N_EVENT + j:
                for q in range(2):
                    home_copy(t, q).wait_recv()
                send_own(n_packet, t, False)

    def wait_x(k, tensors=(0, 1, 2)):
        for dist in range(1, N_Z):
            for t in tensors:
                x_arrival(t, k, (z + dist) % N_Z).wait_recv()

    barrier = pltpu.get_barrier_semaphore()
    signal_neighbours(barrier, (core_peer, y_peer, far_peer))

    own_w = [pltpu.make_async_copy(hbm[t].at[e], shard(t, e, z), own_sem.at[t, e])
             for e in range(n_local) for t in range(3)]
    own_x = pltpu.make_async_copy(x_hbm, toks.at[3], own_sem.at[3, 0])
    own_ids = pltpu.make_async_copy(ids_hbm, ids.at[3], own_sem.at[3, 1])
    own_gates = pltpu.make_async_copy(gates_hbm, gates.at[3], own_sem.at[3, 2])
    own_copies = own_w + [own_x, own_ids, own_gates]
    for copy in own_copies:
        copy.start()

    z_peers = (z + N_Z - 1) // N_Z + (2 * N_Z - 2 - z) // N_Z
    pl.semaphore_wait(barrier, 4 + z_peers)

    meta = []
    for slot, peer in ((2, core_peer), (1, y_peer), (0, far_peer)):
        meta.append(remote(ids_hbm, ids.at[slot], meta_send.at[0, slot], meta_recv.at[0, slot], ep=peer))
        meta.append(remote(gates_hbm, gates.at[slot], meta_send.at[1, slot], meta_recv.at[1, slot], ep=peer))
    for copy in meta:
        copy.start()
    for t in range(3):
        send_own(0, t)
    tok_core = remote(x_hbm, toks.at[2], tok_send.at[2], tok_recv.at[2], ep=core_peer)
    tok_y = remote(x_hbm, toks.at[1], tok_send.at[1], tok_recv.at[1], ep=y_peer)
    tok_far = remote(toks.at[1], toks.at[0], tok_send.at[0], tok_recv.at[0], ep=core_peer)
    tok_core.start()
    tok_y.start()

    def zero(i, carry):
        rows = pl.ds(pl.multiple_of(i % N_BLOCK * block, block), block)
        acc[i // N_BLOCK, rows, :] = jnp.zeros((block, acc.shape[2]), jnp.float32)
        return carry

    lax.fori_loop(0, 4 * N_BLOCK, zero, 0)

    for j in range(N_EVENT):
        event(0, j)
    for copy in own_copies:
        copy.wait()
    tok_y.wait_recv()
    tok_far.start()
    for copy in meta:
        copy.wait_recv()
    tok_core.wait_recv()
    for j in range(LEAD):
        event(1, j)
    wait_x(0)
    tok_far.wait_recv()

    def hidden(e, slot, rows):
        x = toks[slot, rows, :]
        a = jnp.dot(x, wg[e], preferred_element_type=jnp.float32)
        b = jnp.dot(x, wu[e], preferred_element_type=jnp.float32)
        return (a * jax.nn.sigmoid(a) * b).astype(jnp.bfloat16)

    def add_output(h, w_down, expert, slot, rows, start, width):
        o = jnp.dot(h, w_down, preferred_element_type=jnp.float32).astype(jnp.bfloat16).astype(jnp.float32)
        chosen = jnp.where(ids[slot, :, rows] == expert, gates[slot, :, rows], 0.0)
        gate = jnp.sum(chosen, axis=0, keepdims=True)
        gate = jnp.broadcast_to(gate, (128, h.shape[0])).T
        for c in range(width // 128):
            cols = pl.ds(start + c * 128, 128)
            acc[slot, rows, cols] += jnp.where(gate > 0, gate * o[:, c * 128:(c + 1) * 128], 0.0)

    def rows_of(row, block):
        return pl.ds(pl.multiple_of(row * block, block), block)

    def compute(e, slot, row, block):
        rows = rows_of(row, block)
        add_output(hidden(e, slot, rows), wd[e], p * n_local + e, slot, rows, 0, acc.shape[2])

    ffn = wg.shape[2]

    def peer_hidden(e, slot, row):
        rows = rows_of(row, block)
        toks[slot - 2, rows, pl.ds(pl.multiple_of(e * ffn, ffn), ffn)] = hidden(e, slot, rows)

    def peer_output(e, slot, n):
        start = pl.multiple_of(shard_at(n) * d_shard, d_shard)
        h = toks[slot - 2, :, pl.ds(pl.multiple_of(e * ffn, ffn), ffn)]
        expert = y_peer * n_local + n_local - 2 + e
        add_output(h, wd[e, :, pl.ds(start, d_shard)], expert, slot, pl.ds(0, n_tok), start, d_shard)

    def shard_at(n):
        return (z + n + z // 2 * (N_Z - 2 * n)) % N_Z

    def columns(n):
        return pl.ds(pl.multiple_of(shard_at(n) * d_shard, d_shard), d_shard)

    def drain(k, own=True, tensors=(0, 1, 2)):
        for t in tensors:
            @pl.when(z > 0)
            def _():
                z_copy(t, k, z, False, own).wait_send()

            @pl.when(z < N_Z - 1)
            def _():
                z_copy(t, k, z, True, own).wait_send()
            for dist in range(1, N_Z):
                left = (z + N_Z - dist) % N_Z
                right = (z + dist) % N_Z

                @pl.when((z + dist < N_Z) & (z > 0))
                def _():
                    z_copy(t, k, right, False, False).wait_send()

                @pl.when((z >= dist) & (z < N_Z - 1))
                def _():
                    z_copy(t, k, left, True, False).wait_send()
                x_copy(t, k, (z + dist) % N_Z).wait_send()

    def events(i, k, steps, first=0, offset=0):
        for j in range(first, N_EVENT):
            if steps[j] >= offset:
                @pl.when(i == steps[j] - offset)
                def _():
                    event(k, j)

    n_step = 4 * N_BLOCK * 2
    last = n_packet - 1

    def packet(k, carry):
        def step(i, carry):
            events(i, k + 1, STEP_OF, LEAD)

            @pl.when((k == 1) & (i == 2))
            def _():
                pl.semaphore_wait(free, 2 + z_peers)
                for t in range(3):
                    for q in range(2):
                        home_copy(t, q).start()
            compute(2 * k + i % 2, i // 2 // N_BLOCK, i // 2 % N_BLOCK, block)
            return carry

        lax.fori_loop(0, n_step, step, 0)

        @pl.when(k == 0)
        def _():
            for j in range(LEAD):
                event(2, j)
            wait_x(1)
            drain(0)
            signal_neighbours(free, (y_peer,))
        return carry

    lax.fori_loop(0, last - 1, packet, 0)

    tail = n_tok // N_TAIL

    def block_of(ref, row):
        return ref.at[pl.ds(row * tail, tail), :]

    def to_core(row):
        return remote(block_of(acc.at[0], row), block_of(from_core, row),
                      sum_send.at[0, row], sum_recv.at[0, row], ep=core_peer)

    def to_core_near(n):
        return remote(acc.at[2, :, columns(n)], from_core.at[:, columns(n)],
                      sum_send.at[2, n], sum_recv.at[2, n], ep=core_peer)

    def to_y(row):
        return remote(block_of(acc.at[1], row), block_of(from_y, row),
                      sum_send.at[1, row], sum_recv.at[1, row], ep=y_peer)

    def far_first(i, carry):
        events(i, last, STEP_OF_LAST)
        compute(2 * last - 2 + r, i % 2, i // 2, block)
        return carry

    lax.fori_loop(0, 2 * N_BLOCK, far_first, 0)
    wait_x(last - 1)

    def far_second(i, carry):
        events(i, last, STEP_OF_LAST, offset=2 * N_BLOCK)
        compute(2 * last - 1 - r, i % 2, i // 2, tail)
        for n in range(N_TAIL):
            @pl.when(i == 2 * n)
            def _():
                to_core(n).start()

            @pl.when(i == 2 * n + 1)
            def _():
                to_core(n).wait_recv()
                rows = slice(n * tail, (n + 1) * tail)
                acc[1, rows, :] += from_core[rows, :]
                to_y(n).start()
                pl.semaphore_signal(credit.at[n], inc=1, device_id={'ep': core_peer}, device_id_type=MESH)
        return carry

    lax.fori_loop(0, 2 * N_TAIL, far_second, 0)

    def near(i, carry):
        events(i, last, STEP_OF_LAST, offset=2 * N_BLOCK + 2 * N_TAIL)
        compute(2 * last - 2 + i % 2, 2 + i // 2 // N_BLOCK, i // 2 % N_BLOCK, block)
        return carry

    lax.fori_loop(0, 4 * N_BLOCK, near, 0)

    def drain_step(k, carry):
        drain(k)
        return carry

    lax.fori_loop(1, last, drain_step, 0)
    for j in range(LEAD):
        event(n_packet, j)
    wait_x(last)

    def home(i, carry):
        events(i, n_packet, STEP_OF_PEER, LEAD)
        compute(2 * last + i % 2, 2 + i // 2 // N_BLOCK, i // 2 % N_BLOCK, block)
        return carry

    lax.fori_loop(0, 4 * N_BLOCK, home, 0)
    for copy in meta + [tok_core, tok_y, tok_far]:
        copy.wait_send()

    def peer_first(i, carry):
        events(i, n_packet, STEP_OF_PEER, LEAD, offset=4 * N_BLOCK)
        peer_hidden(r, 2 + i // N_BLOCK, i % N_BLOCK)
        return carry

    lax.fori_loop(0, 2 * N_BLOCK, peer_first, 0)
    wait_x(n_packet, (0, 1))

    def peer_second(i, carry):
        events(i, n_packet, STEP_OF_PEER, LEAD, offset=6 * N_BLOCK)
        peer_hidden(1 - r, 2 + i // N_BLOCK, i % N_BLOCK)
        return carry

    lax.fori_loop(0, 2 * N_BLOCK, peer_second, 0)
    for n in range(N_TAIL):
        pl.semaphore_wait(credit.at[n], 1)

    def outputs(e, n, complete):
        def output(i, carry):
            peer_output(e, 2 + i, n)
            if complete:
                @pl.when(i == 0)
                def _():
                    to_core_near(n).start()
            return carry

        lax.fori_loop(0, 2, output, 0)

    def finish(n):
        to_core_near(n).wait_recv()
        cols = columns(n)
        y = toks[3, :, cols].astype(jnp.float32) + (acc[3, :, cols] + from_core[:, cols] + from_y[:, cols])
        toks[3, :, cols] = y.astype(jnp.bfloat16)
        copy = pltpu.make_async_copy(toks.at[3, :, cols], out_hbm.at[:, cols], out_sem.at[n])
        copy.start()
        return copy

    outputs(r, 0, False)
    outputs(1 - r, 0, True)
    outputs(r, 1, False)
    event(n_packet, N_EVENT - 1)
    x_arrival(2, n_packet, shard_at(1)).wait_recv()
    outputs(1 - r, 1, True)
    outputs(r, 2, False)
    outputs(r, 3, False)
    x_arrival(2, n_packet, shard_at(2)).wait_recv()
    outputs(1 - r, 2, True)
    drain(last)
    drain(n_packet, False, (0, 1))
    for t in range(3):
        for q in range(2):
            home_copy(t, q).wait_send()
    for n in range(N_TAIL):
        to_y(n).wait_recv()
        to_core(n).wait_send()
        to_y(n).wait_send()
    outs = [finish(n) for n in range(2)]
    x_arrival(2, n_packet, shard_at(3)).wait_recv()
    outputs(1 - r, 3, True)
    outs += [finish(n) for n in range(2, N_Z)]
    drain(n_packet, False, (2,))
    for n in range(N_Z):
        to_core_near(n).wait_send()
    for copy in outs:
        copy.wait()


def solution(mesh):
    tok_spec = P(('rep', 'fsdp', 'ep'), None)

    def device_step(x_blk, ids_blk, gate_blk, wg_blk, wu_blk, wd_blk):
        n_tok, d_model = x_blk.shape
        n_choice = ids_blk.shape[1]
        n_local, d_shard, ffn = wg_blk.shape
        dma = pltpu.SemaphoreType.DMA
        n_packet = n_local // 2
        any_space = pl.BlockSpec(memory_space=pl.ANY)
        flops = 4 * n_tok * n_local * 6 * d_model * ffn
        return pl.pallas_call(
            moe_kernel,
            out_shape=jax.ShapeDtypeStruct((n_tok, d_model), jnp.bfloat16),
            in_specs=[any_space] * 6,
            out_specs=any_space,
            scratch_shapes=[
                pltpu.VMEM((n_local, d_model, ffn), jnp.bfloat16),
                pltpu.VMEM((n_local, d_model, ffn), jnp.bfloat16),
                pltpu.VMEM((n_local, ffn, d_model), jnp.bfloat16),
                pltpu.VMEM((4, n_tok, d_model), jnp.bfloat16),
                pltpu.VMEM((4, n_choice, n_tok), jnp.int32),
                pltpu.VMEM((4, n_choice, n_tok), jnp.float32),
                pltpu.VMEM((4, n_tok, d_model), jnp.float32),
                pltpu.VMEM((n_tok, d_model), jnp.float32),
                pltpu.VMEM((n_tok, d_model), jnp.float32),
                dma((4, n_local)),
                dma((3, n_packet + 1, N_Z)),
                dma((3, n_packet + 1, N_Z)),
                dma((3, n_packet + 1, N_Z)),
                dma((3, n_packet + 1, N_Z)),
                dma((3, n_packet + 1, N_Z)),
                dma((3,)),
                dma((3,)),
                dma((2, 3)),
                dma((2, 3)),
                dma((3, 2)),
                dma((3, 2)),
                pltpu.SemaphoreType.REGULAR,
                dma((3, N_TAIL)),
                dma((3, N_TAIL)),
                pltpu.SemaphoreType.REGULAR((N_TAIL,)),
                dma((N_TAIL,)),
            ],
            compiler_params=pltpu.CompilerParams(
                collective_id=0, has_side_effects=True, vmem_limit_bytes=67043328),
            cost_estimate=pl.CostEstimate(flops=flops, bytes_accessed=32 << 20, transcendentals=0),
            name='moe',
        )(x_blk, ids_blk.T, gate_blk.T, wg_blk, wu_blk, wd_blk)

    return jax.shard_map(
        device_step, mesh=mesh,
        in_specs=(tok_spec, tok_spec, tok_spec, P('ep', 'fsdp', None), P('ep', 'fsdp', None), P('ep', None, 'fsdp')),
        out_specs=tok_spec, check_vma=False)
```

```python
import functools

import jax
import jax.numpy as jnp
from jax import lax
from jax.experimental import pallas as pl
from jax.experimental.pallas import tpu as pltpu
from jax.sharding import PartitionSpec as P

MESH = pl.DeviceIdType.MESH
N_Z = 4
N_BLOCK = 2
N_TAIL = 4
N_EVENT = 9
LEAD = 2
N_PART = 4
STEP_OF = (0, 0, 3, 4, 6, 9, 12, 13, 15)
STEP_OF_LAST = (2, 5, 6, 6, 8, 11, 12, 15, 17)
STEP_OF_PEER = (0, 0, 1, 3, 5, 8, 10, 14, 16)
OWN_AFTER = (5, 6, 7)
PEER_OWN_AFTER = (6, 10, 13)


def moe_kernel(x_hbm, ids_hbm, gates_hbm, wg_hbm, wu_hbm, wd_hbm, out_ref,
               wg, wu, wd, toks, ids, gates, acc, from_core, from_y,
               own_sem, recv_z, recv_x, send_r, send_l, send_x,
               tok_send, tok_recv, meta_send, meta_recv, home_send, home_recv, free,
               sum_send, sum_recv, credit):
    r = lax.axis_index('rep')
    z = lax.axis_index('fsdp')
    p = lax.axis_index('ep')
    core = p % 2
    core_peer = p + 1 - 2 * core
    y_peer = (p + 2) % 4
    far_peer = (core_peer + 2) % 4
    n_local = wg_hbm.shape[0]
    n_packet = n_local // 2
    d_shard = wg_hbm.shape[1]
    n_tok = x_hbm.shape[0]
    block = n_tok // N_BLOCK

    hbm = (wg_hbm, wu_hbm, wd_hbm)

    def shard(t, e, s, k=0):
        start = pl.multiple_of(s * d_shard, d_shard)
        if is_peer(k) and t >= 2:
            part = wd.shape[1] // N_PART
            return wd.at[e, pl.ds((t - 2) * part, part), pl.ds(start, d_shard)]
        if t == 2:
            return wd.at[e, :, pl.ds(start, d_shard)]
        return (wg, wu)[t].at[e, pl.ds(start, d_shard), :]

    def is_peer(k):
        return isinstance(k, int) and k == n_packet

    def parts(k, t):
        return range(2, 2 + N_PART) if is_peer(k) and t == 2 else (t,)

    def remote(src, dst, send_sem, recv_sem, **where):
        return pltpu.make_async_remote_copy(src_ref=src, dst_ref=dst, send_sem=send_sem, recv_sem=recv_sem,
                                            device_id=where, device_id_type=MESH)

    def place(k):
        return 2 * (k % n_packet)

    def z_copy(t, k, s, right, own):
        here = shard(t, place(k) + r, s, k)
        src = hbm[t].at[place(k) + r] if own else here
        send = send_r if right else send_l
        to = (z + 1) % N_Z if right else (z + N_Z - 1) % N_Z
        return remote(src, here, send.at[t, k, s], recv_z.at[t, k, s], fsdp=to)

    def x_copy(t, k, s):
        here = shard(t, place(k) + r, s, k)
        return remote(here, here, send_x.at[t, k, s], recv_x.at[t, k, s], rep=1 - r)

    def x_arrival(t, k, s):
        here = shard(t, place(k) + 1 - r, s, k)
        return remote(here, here, send_x.at[t, k, s], recv_x.at[t, k, s], rep=1 - r)

    def home_copy(t, q):
        return remote(hbm[t].at[n_local - 2 + q], shard(t, q, z), home_send.at[t, q], home_recv.at[t, q], ep=y_peer)

    def send_own(k, t, own=True):
        @pl.when(z > 0)
        def _():
            for u in parts(k, t):
                z_copy(u, k, z, False, own).start()

        @pl.when(z < N_Z - 1)
        def _():
            for u in parts(k, t):
                z_copy(u, k, z, True, own).start()

    def signal_neighbours(sem, peers):
        for peer in peers:
            pl.semaphore_signal(sem, inc=1, device_id={'ep': peer}, device_id_type=MESH)
        pl.semaphore_signal(sem, inc=1, device_id={'rep': 1 - r}, device_id_type=MESH)

        @pl.when(z > 0)
        def _():
            pl.semaphore_signal(sem, inc=1, device_id={'fsdp': (z + N_Z - 1) % N_Z}, device_id_type=MESH)

        @pl.when(z < N_Z - 1)
        def _():
            pl.semaphore_signal(sem, inc=1, device_id={'fsdp': (z + 1) % N_Z}, device_id_type=MESH)

    def event(k, j):
        dist, t = (j % 3 + 1, j // 3) if is_peer(k) else (j // 3 + 1, j % 3)
        left = (z + N_Z - dist) % N_Z
        right = (z + dist) % N_Z
        for u in parts(k, t):
            @pl.when(z + dist < N_Z)
            def _():
                z_copy(u, k, right, False, False).wait_recv()

                @pl.when(z > 0)
                def _():
                    z_copy(u, k, right, False, False).start()
                x_copy(u, k, right).start()

            @pl.when(z >= dist)
            def _():
                z_copy(u, k, left, True, False).wait_recv()

                @pl.when(z < N_Z - 1)
                def _():
                    z_copy(u, k, left, True, False).start()
                x_copy(u, k, left).start()

        last_packets = isinstance(k, int) and k >= n_packet - 1
        for t in range(3):
            if not last_packets and OWN_AFTER[t] == j:
                send_own(k + 1, t)
            if last_packets and PEER_OWN_AFTER[t] == (k - n_packet + 1) * N_EVENT + j:
                for q in range(2):
                    home_copy(t, q).wait_recv()
                send_own(n_packet, t, False)

    def wait_x(k, tensors=(0, 1, 2)):
        for dist in range(1, N_Z):
            for t in tensors:
                x_arrival(t, k, (z + dist) % N_Z).wait_recv()

    barrier = pltpu.get_barrier_semaphore()
    signal_neighbours(barrier, (core_peer, y_peer, far_peer))

    own_w = [pltpu.make_async_copy(hbm[t].at[e], shard(t, e, z), own_sem.at[t, e])
             for e in range(n_local) for t in range(3)]
    own_x = pltpu.make_async_copy(x_hbm, toks.at[3], own_sem.at[3, 0])
    own_ids = pltpu.make_async_copy(ids_hbm, ids.at[3], own_sem.at[3, 1])
    own_gates = pltpu.make_async_copy(gates_hbm, gates.at[3], own_sem.at[3, 2])
    own_copies = own_w + [own_x, own_ids, own_gates]
    for copy in own_copies:
        copy.start()

    z_peers = (z + N_Z - 1) // N_Z + (2 * N_Z - 2 - z) // N_Z
    pl.semaphore_wait(barrier, 4 + z_peers)

    meta = []
    for slot, peer in ((2, core_peer), (1, y_peer), (0, far_peer)):
        meta.append(remote(ids_hbm, ids.at[slot], meta_send.at[0, slot], meta_recv.at[0, slot], ep=peer))
        meta.append(remote(gates_hbm, gates.at[slot], meta_send.at[1, slot], meta_recv.at[1, slot], ep=peer))
    for copy in meta:
        copy.start()
    for t in range(3):
        send_own(0, t)
    tok_core = remote(x_hbm, toks.at[2], tok_send.at[2], tok_recv.at[2], ep=core_peer)
    tok_y = remote(x_hbm, toks.at[1], tok_send.at[1], tok_recv.at[1], ep=y_peer)
    tok_far = remote(toks.at[1], toks.at[0], tok_send.at[0], tok_recv.at[0], ep=core_peer)
    tok_core.start()
    tok_y.start()

    def zero(i, carry):
        rows = pl.ds(pl.multiple_of(i % N_BLOCK * block, block), block)
        acc[i // N_BLOCK, rows, :] = jnp.zeros((block, acc.shape[2]), jnp.float32)
        return carry

    lax.fori_loop(0, 4 * N_BLOCK, zero, 0)

    for j in range(N_EVENT):
        event(0, j)
    for copy in own_copies:
        copy.wait()
    tok_y.wait_recv()
    tok_far.start()
    for copy in meta:
        copy.wait_recv()
    tok_core.wait_recv()
    for j in range(LEAD):
        event(1, j)
    wait_x(0)
    tok_far.wait_recv()

    def hidden(e, slot, rows):
        x = toks[slot, rows, :]
        a = jnp.dot(x, wg[e], preferred_element_type=jnp.float32)
        b = jnp.dot(x, wu[e], preferred_element_type=jnp.float32)
        return (a * jax.nn.sigmoid(a) * b).astype(jnp.bfloat16)

    def add_output(h, w_down, expert, slot, rows, start, width):
        o = jnp.dot(h, w_down, preferred_element_type=jnp.float32).astype(jnp.bfloat16).astype(jnp.float32)
        chosen = jnp.where(ids[slot, :, rows] == expert, gates[slot, :, rows], 0.0)
        gate = jnp.sum(chosen, axis=0, keepdims=True)
        gate = jnp.broadcast_to(gate, (128, h.shape[0])).T
        for c in range(width // 128):
            cols = pl.ds(start + c * 128, 128)
            acc[slot, rows, cols] += jnp.where(gate > 0, gate * o[:, c * 128:(c + 1) * 128], 0.0)

    def rows_of(row, block):
        return pl.ds(pl.multiple_of(row * block, block), block)

    def compute(e, slot, row, block):
        rows = rows_of(row, block)
        add_output(hidden(e, slot, rows), wd[e], p * n_local + e, slot, rows, 0, acc.shape[2])

    ffn = wg.shape[2]

    def peer_hidden(e, slot, row):
        rows = rows_of(row, block)
        toks[slot - 2, rows, pl.ds(pl.multiple_of(e * ffn, ffn), ffn)] = hidden(e, slot, rows)

    def peer_output(e, slot, n):
        start = pl.multiple_of(shard_at(n) * d_shard, d_shard)
        h = toks[slot - 2, :, pl.ds(pl.multiple_of(e * ffn, ffn), ffn)]
        expert = y_peer * n_local + n_local - 2 + e
        add_output(h, wd[e, :, pl.ds(start, d_shard)], expert, slot, pl.ds(0, n_tok), start, d_shard)

    def shard_at(n):
        return (z + n + z // 2 * (N_Z - 2 * n)) % N_Z

    def columns(n):
        return pl.ds(pl.multiple_of(shard_at(n) * d_shard, d_shard), d_shard)

    def drain(k, own=True, tensors=(0, 1, 2)):
        for t in [u for t in tensors for u in parts(k, t)]:
            @pl.when(z > 0)
            def _():
                z_copy(t, k, z, False, own).wait_send()

            @pl.when(z < N_Z - 1)
            def _():
                z_copy(t, k, z, True, own).wait_send()
            for dist in range(1, N_Z):
                left = (z + N_Z - dist) % N_Z
                right = (z + dist) % N_Z

                @pl.when((z + dist < N_Z) & (z > 0))
                def _():
                    z_copy(t, k, right, False, False).wait_send()

                @pl.when((z >= dist) & (z < N_Z - 1))
                def _():
                    z_copy(t, k, left, True, False).wait_send()
                x_copy(t, k, (z + dist) % N_Z).wait_send()

    def events(i, k, steps, first=0, offset=0):
        for j in range(first, N_EVENT):
            if steps[j] >= offset:
                @pl.when(i == steps[j] - offset)
                def _():
                    event(k, j)

    n_step = 4 * N_BLOCK * 2
    last = n_packet - 1

    def packet(k, carry):
        def step(i, carry):
            events(i, k + 1, STEP_OF, LEAD)

            @pl.when((k == 1) & (i == 2))
            def _():
                pl.semaphore_wait(free, 2 + z_peers)
                for t in range(3):
                    for q in range(2):
                        home_copy(t, q).start()
            compute(2 * k + i % 2, i // 2 // N_BLOCK, i // 2 % N_BLOCK, block)
            return carry

        lax.fori_loop(0, n_step, step, 0)

        @pl.when(k == 0)
        def _():
            for j in range(LEAD):
                event(2, j)
            wait_x(1)
            drain(0)
            signal_neighbours(free, (y_peer,))
        return carry

    lax.fori_loop(0, last - 1, packet, 0)

    tail = n_tok // N_TAIL

    def block_of(ref, row):
        return ref.at[pl.ds(row * tail, tail), :]

    def to_core(row):
        return remote(block_of(acc.at[0], row), block_of(from_core, row),
                      sum_send.at[0, row], sum_recv.at[0, row], ep=core_peer)

    def to_core_near(n):
        return remote(acc.at[2, :, columns(n)], from_core.at[:, columns(n)],
                      sum_send.at[2, n], sum_recv.at[2, n], ep=core_peer)

    def to_y(row):
        return remote(block_of(acc.at[1], row), block_of(from_y, row),
                      sum_send.at[1, row], sum_recv.at[1, row], ep=y_peer)

    def far_first(i, carry):
        events(i, last, STEP_OF_LAST)
        compute(2 * last - 2 + r, i % 2, i // 2, block)
        return carry

    lax.fori_loop(0, 2 * N_BLOCK, far_first, 0)
    wait_x(last - 1)

    def far_second(i, carry):
        events(i, last, STEP_OF_LAST, offset=2 * N_BLOCK)
        compute(2 * last - 1 - r, i % 2, i // 2, tail)
        for n in range(N_TAIL):
            @pl.when(i == 2 * n)
            def _():
                to_core(n).start()

            @pl.when(i == 2 * n + 1)
            def _():
                to_core(n).wait_recv()
                rows = slice(n * tail, (n + 1) * tail)
                acc[1, rows, :] += from_core[rows, :]
                to_y(n).start()
                pl.semaphore_signal(credit.at[n], inc=1, device_id={'ep': core_peer}, device_id_type=MESH)
        return carry

    lax.fori_loop(0, 2 * N_TAIL, far_second, 0)

    def near(i, carry):
        events(i, last, STEP_OF_LAST, offset=2 * N_BLOCK + 2 * N_TAIL)
        compute(2 * last - 2 + i % 2, 2 + i // 2 // N_BLOCK, i // 2 % N_BLOCK, block)
        return carry

    lax.fori_loop(0, 4 * N_BLOCK, near, 0)

    def drain_step(k, carry):
        drain(k)
        return carry

    lax.fori_loop(1, last, drain_step, 0)
    for j in range(LEAD):
        event(n_packet, j)
    wait_x(last)

    def home(i, carry):
        events(i, n_packet, STEP_OF_PEER, LEAD)
        compute(2 * last + i % 2, 2 + i // 2 // N_BLOCK, i // 2 % N_BLOCK, block)
        return carry

    lax.fori_loop(0, 4 * N_BLOCK, home, 0)
    for copy in meta + [tok_core, tok_y, tok_far]:
        copy.wait_send()

    def peer_first(i, carry):
        events(i, n_packet, STEP_OF_PEER, LEAD, offset=4 * N_BLOCK)
        peer_hidden(r, 2 + i // N_BLOCK, i % N_BLOCK)
        return carry

    lax.fori_loop(0, 2 * N_BLOCK, peer_first, 0)
    wait_x(n_packet, (0, 1))

    def peer_second(i, carry):
        events(i, n_packet, STEP_OF_PEER, LEAD, offset=6 * N_BLOCK)
        peer_hidden(1 - r, 2 + i // N_BLOCK, i % N_BLOCK)
        return carry

    lax.fori_loop(0, 2 * N_BLOCK, peer_second, 0)
    for n in range(N_TAIL):
        pl.semaphore_wait(credit.at[n], 1)

    def outputs(e, n, complete):
        def output(i, carry):
            peer_output(e, 2 + i, n)
            if complete:
                @pl.when(i == 0)
                def _():
                    to_core_near(n).start()
            return carry

        lax.fori_loop(0, 2, output, 0)

    def finish(n):
        to_core_near(n).wait_recv()
        cols = columns(n)
        y = toks[3, :, cols].astype(jnp.float32) + (acc[3, :, cols] + from_core[:, cols] + from_y[:, cols])
        out_ref[:, cols] = y.astype(jnp.bfloat16)

    def wait_down(n):
        for u in parts(n_packet, 2):
            x_arrival(u, n_packet, shard_at(n)).wait_recv()

    outputs(r, 0, False)
    event(n_packet, N_EVENT - 1)
    outputs(1 - r, 0, True)
    outputs(r, 1, False)
    wait_down(1)
    outputs(1 - r, 1, True)
    outputs(r, 2, False)
    outputs(r, 3, False)
    wait_down(2)
    outputs(1 - r, 2, True)
    drain(last)
    drain(n_packet, False, (0, 1))
    for t in range(3):
        for q in range(2):
            home_copy(t, q).wait_send()
    for n in range(N_TAIL):
        to_y(n).wait_recv()
        to_core(n).wait_send()
        to_y(n).wait_send()
    for n in range(2):
        finish(n)
    wait_down(3)
    outputs(1 - r, 3, True)
    for n in range(2, N_Z):
        finish(n)
    drain(n_packet, False, (2,))
    for n in range(N_Z):
        to_core_near(n).wait_send()


def solution(mesh):
    tok_spec = P(('rep', 'fsdp', 'ep'), None)

    def device_step(x_blk, ids_blk, gate_blk, wg_blk, wu_blk, wd_blk):
        n_tok, d_model = x_blk.shape
        n_choice = ids_blk.shape[1]
        n_local, d_shard, ffn = wg_blk.shape
        dma = pltpu.SemaphoreType.DMA
        n_packet = n_local // 2
        any_space = pl.BlockSpec(memory_space=pl.ANY)
        flops = 4 * n_tok * n_local * 6 * d_model * ffn
        return pl.pallas_call(
            moe_kernel,
            out_shape=pltpu.VMEM((n_tok, d_model), jnp.bfloat16),
            in_specs=[any_space] * 6,
            out_specs=pl.BlockSpec(memory_space=pltpu.VMEM),
            scratch_shapes=[
                pltpu.VMEM((n_local, d_model, ffn), jnp.bfloat16),
                pltpu.VMEM((n_local, d_model, ffn), jnp.bfloat16),
                pltpu.VMEM((n_local, ffn, d_model), jnp.bfloat16),
                pltpu.VMEM((4, n_tok, d_model), jnp.bfloat16),
                pltpu.VMEM((4, n_choice, n_tok), jnp.int32),
                pltpu.VMEM((4, n_choice, n_tok), jnp.float32),
                pltpu.VMEM((4, n_tok, d_model), jnp.float32),
                pltpu.VMEM((n_tok, d_model), jnp.float32),
                pltpu.VMEM((n_tok, d_model), jnp.float32),
                dma((4, n_local)),
                dma((2 + N_PART, n_packet + 1, N_Z)),
                dma((2 + N_PART, n_packet + 1, N_Z)),
                dma((2 + N_PART, n_packet + 1, N_Z)),
                dma((2 + N_PART, n_packet + 1, N_Z)),
                dma((2 + N_PART, n_packet + 1, N_Z)),
                dma((3,)),
                dma((3,)),
                dma((2, 3)),
                dma((2, 3)),
                dma((3, 2)),
                dma((3, 2)),
                pltpu.SemaphoreType.REGULAR,
                dma((3, N_TAIL)),
                dma((3, N_TAIL)),
                pltpu.SemaphoreType.REGULAR((N_TAIL,)),
            ],
            compiler_params=pltpu.CompilerParams(
                collective_id=0, has_side_effects=True, vmem_limit_bytes=62914560),
            cost_estimate=pl.CostEstimate(flops=flops, bytes_accessed=32 << 20, transcendentals=0),
            name='moe',
        )(x_blk, ids_blk.T, gate_blk.T, wg_blk, wu_blk, wd_blk)

    return jax.shard_map(
        device_step, mesh=mesh,
        in_specs=(tok_spec, tok_spec, tok_spec, P('ep', 'fsdp', None), P('ep', 'fsdp', None), P('ep', None, 'fsdp')),
        out_specs=tok_spec, check_vma=False)
```

```python
import functools

import jax
import jax.numpy as jnp
from jax import lax
from jax.experimental import pallas as pl
from jax.experimental.pallas import tpu as pltpu
from jax.sharding import PartitionSpec as P

MESH = pl.DeviceIdType.MESH
N_Z = 4
N_BLOCK = 2
N_TAIL = 4
N_EVENT = 9
LEAD = 2
N_PART = 1
STEP_OF = (0, 0, 3, 4, 6, 9, 12, 13, 15)
STEP_OF_LAST = (2, 5, 6, 6, 8, 11, 12, 15, 17)
STEP_OF_PEER = (0, 0, 1, 3, 5, 8, 12, 15, 17)
OWN_AFTER = (5, 6, 7)
PEER_OWN_AFTER = (6, 10, 13)


def moe_kernel(x_hbm, ids_hbm, gates_hbm, wg_hbm, wu_hbm, wd_hbm, out_ref,
               wg, wu, wd, toks, ids, gates, acc, from_core, from_y,
               own_sem, recv_z, recv_x, send_r, send_l, send_x,
               tok_send, tok_recv, meta_send, meta_recv, home_send, home_recv, free,
               sum_send, sum_recv, credit):
    r = lax.axis_index('rep')
    z = lax.axis_index('fsdp')
    p = lax.axis_index('ep')
    core = p % 2
    core_peer = p + 1 - 2 * core
    y_peer = (p + 2) % 4
    far_peer = (core_peer + 2) % 4
    n_local = wg_hbm.shape[0]
    n_packet = n_local // 2
    d_shard = wg_hbm.shape[1]
    n_tok = x_hbm.shape[0]
    block = n_tok // N_BLOCK

    hbm = (wg_hbm, wu_hbm, wd_hbm)

    def shard(t, e, s, k=0):
        start = pl.multiple_of(s * d_shard, d_shard)
        if is_peer(k) and t >= 2:
            part = wd.shape[1] // N_PART
            return wd.at[e, pl.ds((t - 2) * part, part), pl.ds(start, d_shard)]
        if t == 2:
            return wd.at[e, :, pl.ds(start, d_shard)]
        return (wg, wu)[t].at[e, pl.ds(start, d_shard), :]

    def is_peer(k):
        return isinstance(k, int) and k == n_packet

    def parts(k, t):
        return range(2, 2 + N_PART) if is_peer(k) and t == 2 else (t,)

    def remote(src, dst, send_sem, recv_sem, **where):
        return pltpu.make_async_remote_copy(src_ref=src, dst_ref=dst, send_sem=send_sem, recv_sem=recv_sem,
                                            device_id=where, device_id_type=MESH)

    def place(k):
        return 2 * (k % n_packet)

    def z_copy(t, k, s, right, own):
        here = shard(t, place(k) + r, s, k)
        src = hbm[t].at[place(k) + r] if own else here
        send = send_r if right else send_l
        to = (z + 1) % N_Z if right else (z + N_Z - 1) % N_Z
        return remote(src, here, send.at[t, k, s], recv_z.at[t, k, s], fsdp=to)

    def x_copy(t, k, s):
        here = shard(t, place(k) + r, s, k)
        return remote(here, here, send_x.at[t, k, s], recv_x.at[t, k, s], rep=1 - r)

    def x_arrival(t, k, s):
        here = shard(t, place(k) + 1 - r, s, k)
        return remote(here, here, send_x.at[t, k, s], recv_x.at[t, k, s], rep=1 - r)

    def home_copy(t, q):
        return remote(hbm[t].at[n_local - 2 + q], shard(t, q, z), home_send.at[t, q], home_recv.at[t, q], ep=y_peer)

    def send_own(k, t, own=True):
        @pl.when(z > 0)
        def _():
            for u in parts(k, t):
                z_copy(u, k, z, False, own).start()

        @pl.when(z < N_Z - 1)
        def _():
            for u in parts(k, t):
                z_copy(u, k, z, True, own).start()

    def signal_neighbours(sem, peers):
        for peer in peers:
            pl.semaphore_signal(sem, inc=1, device_id={'ep': peer}, device_id_type=MESH)
        pl.semaphore_signal(sem, inc=1, device_id={'rep': 1 - r}, device_id_type=MESH)

        @pl.when(z > 0)
        def _():
            pl.semaphore_signal(sem, inc=1, device_id={'fsdp': (z + N_Z - 1) % N_Z}, device_id_type=MESH)

        @pl.when(z < N_Z - 1)
        def _():
            pl.semaphore_signal(sem, inc=1, device_id={'fsdp': (z + 1) % N_Z}, device_id_type=MESH)

    def event(k, j):
        dist, t = (j % 3 + 1, j // 3) if is_peer(k) else (j // 3 + 1, j % 3)
        left = (z + N_Z - dist) % N_Z
        right = (z + dist) % N_Z
        for u in parts(k, t):
            @pl.when(z + dist < N_Z)
            def _():
                z_copy(u, k, right, False, False).wait_recv()

                @pl.when(z > 0)
                def _():
                    z_copy(u, k, right, False, False).start()
                x_copy(u, k, right).start()

            @pl.when(z >= dist)
            def _():
                z_copy(u, k, left, True, False).wait_recv()

                @pl.when(z < N_Z - 1)
                def _():
                    z_copy(u, k, left, True, False).start()
                x_copy(u, k, left).start()

        last_packets = isinstance(k, int) and k >= n_packet - 1
        for t in range(3):
            if not last_packets and OWN_AFTER[t] == j:
                send_own(k + 1, t)
            if last_packets and PEER_OWN_AFTER[t] == (k - n_packet + 1) * N_EVENT + j:
                for q in range(2):
                    home_copy(t, q).wait_recv()
                send_own(n_packet, t, False)

    def wait_x(k, tensors=(0, 1, 2)):
        for dist in range(1, N_Z):
            for t in tensors:
                x_arrival(t, k, (z + dist) % N_Z).wait_recv()

    barrier = pltpu.get_barrier_semaphore()
    signal_neighbours(barrier, (core_peer, y_peer, far_peer))

    own_w = [pltpu.make_async_copy(hbm[t].at[e], shard(t, e, z), own_sem.at[t, e])
             for e in range(n_local) for t in range(3)]
    own_x = pltpu.make_async_copy(x_hbm, toks.at[3], own_sem.at[3, 0])
    own_ids = pltpu.make_async_copy(ids_hbm, ids.at[3], own_sem.at[3, 1])
    own_gates = pltpu.make_async_copy(gates_hbm, gates.at[3], own_sem.at[3, 2])
    own_copies = own_w + [own_x, own_ids, own_gates]
    for copy in own_copies:
        copy.start()

    z_peers = (z + N_Z - 1) // N_Z + (2 * N_Z - 2 - z) // N_Z
    pl.semaphore_wait(barrier, 4 + z_peers)

    meta = []
    for slot, peer in ((2, core_peer), (1, y_peer), (0, far_peer)):
        meta.append(remote(ids_hbm, ids.at[slot], meta_send.at[0, slot], meta_recv.at[0, slot], ep=peer))
        meta.append(remote(gates_hbm, gates.at[slot], meta_send.at[1, slot], meta_recv.at[1, slot], ep=peer))
    for copy in meta:
        copy.start()
    for t in range(3):
        send_own(0, t)
    tok_core = remote(x_hbm, toks.at[2], tok_send.at[2], tok_recv.at[2], ep=core_peer)
    tok_y = remote(x_hbm, toks.at[1], tok_send.at[1], tok_recv.at[1], ep=y_peer)
    tok_far = remote(toks.at[1], toks.at[0], tok_send.at[0], tok_recv.at[0], ep=core_peer)
    tok_core.start()
    tok_y.start()

    def zero(i, carry):
        rows = pl.ds(pl.multiple_of(i % N_BLOCK * block, block), block)
        acc[i // N_BLOCK, rows, :] = jnp.zeros((block, acc.shape[2]), jnp.float32)
        return carry

    lax.fori_loop(0, 4 * N_BLOCK, zero, 0)

    for j in range(N_EVENT):
        event(0, j)
    for copy in own_copies:
        copy.wait()
    tok_y.wait_recv()
    tok_far.start()
    for copy in meta:
        copy.wait_recv()
    tok_core.wait_recv()
    for j in range(LEAD):
        event(1, j)
    wait_x(0)
    tok_far.wait_recv()

    def hidden(e, slot, rows):
        x = toks[slot, rows, :]
        a = jnp.dot(x, wg[e], preferred_element_type=jnp.float32)
        b = jnp.dot(x, wu[e], preferred_element_type=jnp.float32)
        return (a * jax.nn.sigmoid(a) * b).astype(jnp.bfloat16)

    def add_output(h, w_down, expert, slot, rows, start, width):
        o = jnp.dot(h, w_down, preferred_element_type=jnp.float32).astype(jnp.bfloat16).astype(jnp.float32)
        chosen = jnp.where(ids[slot, :, rows] == expert, gates[slot, :, rows], 0.0)
        gate = jnp.sum(chosen, axis=0, keepdims=True)
        gate = jnp.broadcast_to(gate, (128, h.shape[0])).T
        for c in range(width // 128):
            cols = pl.ds(start + c * 128, 128)
            acc[slot, rows, cols] += jnp.where(gate > 0, gate * o[:, c * 128:(c + 1) * 128], 0.0)

    def rows_of(row, block):
        return pl.ds(pl.multiple_of(row * block, block), block)

    def compute(e, slot, row, block):
        rows = rows_of(row, block)
        add_output(hidden(e, slot, rows), wd[e], p * n_local + e, slot, rows, 0, acc.shape[2])

    ffn = wg.shape[2]

    def peer_hidden(e, slot, row):
        rows = rows_of(row, block)
        toks[slot - 2, rows, pl.ds(pl.multiple_of(e * ffn, ffn), ffn)] = hidden(e, slot, rows)

    def peer_output(e, slot, n):
        start = pl.multiple_of(shard_at(n) * d_shard, d_shard)
        h = toks[slot - 2, :, pl.ds(pl.multiple_of(e * ffn, ffn), ffn)]
        expert = y_peer * n_local + n_local - 2 + e
        add_output(h, wd[e, :, pl.ds(start, d_shard)], expert, slot, pl.ds(0, n_tok), start, d_shard)

    def shard_at(n):
        odd, upper = z % 2, z // 2
        return (z, 1 + odd + 2 * upper - 2 * odd * upper, 2 - 2 * odd - upper + 2 * odd * upper, 3 - 3 * upper)[n]

    def columns(n):
        return pl.ds(pl.multiple_of(shard_at(n) * d_shard, d_shard), d_shard)

    def drain(k, own=True, tensors=(0, 1, 2)):
        for t in [u for t in tensors for u in parts(k, t)]:
            @pl.when(z > 0)
            def _():
                z_copy(t, k, z, False, own).wait_send()

            @pl.when(z < N_Z - 1)
            def _():
                z_copy(t, k, z, True, own).wait_send()
            for dist in range(1, N_Z):
                left = (z + N_Z - dist) % N_Z
                right = (z + dist) % N_Z

                @pl.when((z + dist < N_Z) & (z > 0))
                def _():
                    z_copy(t, k, right, False, False).wait_send()

                @pl.when((z >= dist) & (z < N_Z - 1))
                def _():
                    z_copy(t, k, left, True, False).wait_send()
                x_copy(t, k, (z + dist) % N_Z).wait_send()

    def events(i, k, steps, first=0, offset=0):
        for j in range(first, N_EVENT):
            if steps[j] >= offset:
                @pl.when(i == steps[j] - offset)
                def _():
                    event(k, j)

    n_step = 4 * N_BLOCK * 2
    last = n_packet - 1

    def packet(k, carry):
        def step(i, carry):
            events(i, k + 1, STEP_OF, LEAD)

            @pl.when((k == 1) & (i == 2))
            def _():
                pl.semaphore_wait(free, 2 + z_peers)
                for t in range(3):
                    for q in range(2):
                        home_copy(t, q).start()
            compute(2 * k + i % 2, i // 2 // N_BLOCK, i // 2 % N_BLOCK, block)
            return carry

        lax.fori_loop(0, n_step, step, 0)

        @pl.when(k == 0)
        def _():
            for j in range(LEAD):
                event(2, j)
            wait_x(1)
            drain(0)
            signal_neighbours(free, (y_peer,))
        return carry

    lax.fori_loop(0, last - 1, packet, 0)

    tail = n_tok // N_TAIL

    def block_of(ref, row):
        return ref.at[pl.ds(row * tail, tail), :]

    def to_core(row):
        return remote(block_of(acc.at[0], row), block_of(from_core, row),
                      sum_send.at[0, row], sum_recv.at[0, row], ep=core_peer)

    def to_core_near(n):
        return remote(acc.at[2, :, columns(n)], from_core.at[:, columns(n)],
                      sum_send.at[2, n], sum_recv.at[2, n], ep=core_peer)

    def to_y(row):
        return remote(block_of(acc.at[1], row), block_of(from_y, row),
                      sum_send.at[1, row], sum_recv.at[1, row], ep=y_peer)

    def far_first(i, carry):
        events(i, last, STEP_OF_LAST)
        compute(2 * last - 2 + r, i % 2, i // 2, block)
        return carry

    lax.fori_loop(0, 2 * N_BLOCK, far_first, 0)
    wait_x(last - 1)

    def far_second(i, carry):
        events(i, last, STEP_OF_LAST, offset=2 * N_BLOCK)
        compute(2 * last - 1 - r, i % 2, i // 2, tail)
        for n in range(N_TAIL):
            @pl.when(i == 2 * n)
            def _():
                to_core(n).start()

            @pl.when(i == 2 * n + 1)
            def _():
                to_core(n).wait_recv()
                rows = slice(n * tail, (n + 1) * tail)
                acc[1, rows, :] += from_core[rows, :]
                to_y(n).start()
                pl.semaphore_signal(credit.at[n], inc=1, device_id={'ep': core_peer}, device_id_type=MESH)
        return carry

    lax.fori_loop(0, 2 * N_TAIL, far_second, 0)

    def near(i, carry):
        events(i, last, STEP_OF_LAST, offset=2 * N_BLOCK + 2 * N_TAIL)
        compute(2 * last - 2 + i % 2, 2 + i // 2 // N_BLOCK, i // 2 % N_BLOCK, block)
        return carry

    lax.fori_loop(0, 4 * N_BLOCK, near, 0)

    def drain_step(k, carry):
        drain(k)
        return carry

    lax.fori_loop(1, last, drain_step, 0)
    for j in range(LEAD):
        event(n_packet, j)
    wait_x(last)

    def home(i, carry):
        events(i, n_packet, STEP_OF_PEER, LEAD)
        compute(2 * last + i % 2, 2 + i // 2 // N_BLOCK, i // 2 % N_BLOCK, block)
        return carry

    lax.fori_loop(0, 4 * N_BLOCK, home, 0)
    for copy in meta + [tok_core, tok_y, tok_far]:
        copy.wait_send()

    def peer_first(i, carry):
        events(i, n_packet, STEP_OF_PEER, LEAD, offset=4 * N_BLOCK)
        peer_hidden(r, 2 + i // N_BLOCK, i % N_BLOCK)
        return carry

    lax.fori_loop(0, 2 * N_BLOCK, peer_first, 0)
    event(n_packet, 6)
    wait_x(n_packet, (0, 1))

    def peer_second(i, carry):
        events(i, n_packet, STEP_OF_PEER, 7, offset=6 * N_BLOCK)
        peer_hidden(1 - r, 2 + i // N_BLOCK, i % N_BLOCK)
        return carry

    lax.fori_loop(0, 2 * N_BLOCK, peer_second, 0)
    for n in range(N_TAIL):
        pl.semaphore_wait(credit.at[n], 1)

    def outputs(e, n, complete):
        def output(i, carry):
            peer_output(e, 2 + i, n)
            if complete:
                @pl.when(i == 0)
                def _():
                    to_core_near(n).start()
            return carry

        lax.fori_loop(0, 2, output, 0)

    def finish(n):
        to_core_near(n).wait_recv()
        cols = columns(n)
        y = toks[3, :, cols].astype(jnp.float32) + (acc[3, :, cols] + from_core[:, cols] + from_y[:, cols])
        out_ref[:, cols] = y.astype(jnp.bfloat16)

    def wait_down(n):
        for u in parts(n_packet, 2):
            x_arrival(u, n_packet, shard_at(n)).wait_recv()

    outputs(r, 0, False)
    outputs(1 - r, 0, True)
    outputs(r, 1, False)
    event(n_packet, N_EVENT - 1)
    wait_down(1)
    outputs(1 - r, 1, True)
    outputs(r, 2, False)
    outputs(r, 3, False)
    wait_down(2)
    outputs(1 - r, 2, True)
    drain(last)
    drain(n_packet, False, (0, 1))
    for t in range(3):
        for q in range(2):
            home_copy(t, q).wait_send()
    for n in range(N_TAIL):
        to_y(n).wait_recv()
        to_core(n).wait_send()
        to_y(n).wait_send()
    for n in range(2):
        finish(n)
    wait_down(3)
    outputs(1 - r, 3, True)
    for n in range(2, N_Z):
        finish(n)
    drain(n_packet, False, (2,))
    for n in range(N_Z):
        to_core_near(n).wait_send()


def solution(mesh):
    tok_spec = P(('rep', 'fsdp', 'ep'), None)

    def device_step(x_blk, ids_blk, gate_blk, wg_blk, wu_blk, wd_blk):
        n_tok, d_model = x_blk.shape
        n_choice = ids_blk.shape[1]
        n_local, d_shard, ffn = wg_blk.shape
        dma = pltpu.SemaphoreType.DMA
        n_packet = n_local // 2
        any_space = pl.BlockSpec(memory_space=pl.ANY)
        flops = 4 * n_tok * n_local * 6 * d_model * ffn
        return pl.pallas_call(
            moe_kernel,
            out_shape=pltpu.VMEM((n_tok, d_model), jnp.bfloat16),
            in_specs=[any_space] * 6,
            out_specs=pl.BlockSpec(memory_space=pltpu.VMEM),
            scratch_shapes=[
                pltpu.VMEM((n_local, d_model, ffn), jnp.bfloat16),
                pltpu.VMEM((n_local, d_model, ffn), jnp.bfloat16),
                pltpu.VMEM((n_local, ffn, d_model), jnp.bfloat16),
                pltpu.VMEM((4, n_tok, d_model), jnp.bfloat16),
                pltpu.VMEM((4, n_choice, n_tok), jnp.int32),
                pltpu.VMEM((4, n_choice, n_tok), jnp.float32),
                pltpu.VMEM((4, n_tok, d_model), jnp.float32),
                pltpu.VMEM((n_tok, d_model), jnp.float32),
                pltpu.VMEM((n_tok, d_model), jnp.float32),
                dma((4, n_local)),
                dma((2 + N_PART, n_packet + 1, N_Z)),
                dma((2 + N_PART, n_packet + 1, N_Z)),
                dma((2 + N_PART, n_packet + 1, N_Z)),
                dma((2 + N_PART, n_packet + 1, N_Z)),
                dma((2 + N_PART, n_packet + 1, N_Z)),
                dma((3,)),
                dma((3,)),
                dma((2, 3)),
                dma((2, 3)),
                dma((3, 2)),
                dma((3, 2)),
                pltpu.SemaphoreType.REGULAR,
                dma((3, N_TAIL)),
                dma((3, N_TAIL)),
                pltpu.SemaphoreType.REGULAR((N_TAIL,)),
            ],
            compiler_params=pltpu.CompilerParams(
                collective_id=0, has_side_effects=True, vmem_limit_bytes=62914560),
            cost_estimate=pl.CostEstimate(flops=flops, bytes_accessed=32 << 20, transcendentals=0),
            name='moe',
        )(x_blk, ids_blk.T, gate_blk.T, wg_blk, wu_blk, wd_blk)

    return jax.shard_map(
        device_step, mesh=mesh,
        in_specs=(tok_spec, tok_spec, tok_spec, P('ep', 'fsdp', None), P('ep', 'fsdp', None), P('ep', None, 'fsdp')),
        out_specs=tok_spec, check_vma=False)
```

```python
import functools

import jax
import jax.numpy as jnp
from jax import lax
from jax.experimental import pallas as pl
from jax.experimental.pallas import tpu as pltpu
from jax.sharding import PartitionSpec as P

MESH = pl.DeviceIdType.MESH
N_Z = 4
N_BLOCK = 2
N_TAIL = 4
N_EVENT = 9
LEAD = 2
STEP_OF = (0, 0, 3, 4, 6, 9, 12, 13, 15)
STEP_OF_LAST = (2, 5, 6, 6, 8, 11, 12, 15, 17)
STEP_OF_PEER = (0, 0, 1, 3, 5, 8, 12, 15, 17)
OWN_AFTER = (5, 6, 7)
PEER_OWN_AFTER = (6, 10, 13)


def moe_kernel(x_hbm, ids_hbm, gates_hbm, wg_hbm, wu_hbm, wd_hbm, out_ref,
               wg, wu, wd, toks, ids, gates, acc, from_core, from_y,
               own_sem, recv_z, recv_x, send_r, send_l, send_x,
               tok_send, tok_recv, meta_send, meta_recv, home_send, home_recv, free,
               sum_send, sum_recv, credit):
    r = lax.axis_index('rep')
    z = lax.axis_index('fsdp')
    p = lax.axis_index('ep')
    core = p % 2
    core_peer = p + 1 - 2 * core
    y_peer = (p + 2) % 4
    far_peer = (core_peer + 2) % 4
    n_local = wg_hbm.shape[0]
    n_packet = n_local // 2
    d_shard = wg_hbm.shape[1]
    n_tok = x_hbm.shape[0]
    block = n_tok // N_BLOCK

    hbm = (wg_hbm, wu_hbm, wd_hbm)

    def shard(t, e, s, k):
        start = pl.multiple_of(s * d_shard, d_shard)
        if len(parts(k, 2)) > 1 and t >= 2:
            half = wd.shape[1] // 2
            return wd.at[e, pl.ds((t - 2) * half, half), pl.ds(start, d_shard)]
        if len(parts(k, 0)) > 1 and t in (0, 3):
            half = d_shard // 2
            return wg.at[e, pl.ds(pl.multiple_of(start + t // 3 * half, half), half), :]
        if t == 2:
            return wd.at[e, :, pl.ds(start, d_shard)]
        return (wg, wu)[t].at[e, pl.ds(start, d_shard), :]

    def source(t, e, k):
        if len(parts(k, 0)) > 1 and t in (0, 3):
            half = d_shard // 2
            return wg_hbm.at[e, pl.ds(t // 3 * half, half), :]
        return hbm[t].at[e]

    def is_peer(k):
        return isinstance(k, int) and k == n_packet

    def parts(k, t):
        first = isinstance(k, int) and k == 0 and t == 0
        return (t, 3) if first or (is_peer(k) and t == 2) else (t,)

    def remote(src, dst, send_sem, recv_sem, **where):
        return pltpu.make_async_remote_copy(src_ref=src, dst_ref=dst, send_sem=send_sem, recv_sem=recv_sem,
                                            device_id=where, device_id_type=MESH)

    def place(k):
        return 2 * (k % n_packet)

    def z_copy(t, k, s, right, own):
        here = shard(t, place(k) + r, s, k)
        src = source(t, place(k) + r, k) if own else here
        send = send_r if right else send_l
        to = (z + 1) % N_Z if right else (z + N_Z - 1) % N_Z
        return remote(src, here, send.at[t, k, s], recv_z.at[t, k, s], fsdp=to)

    def x_copy(t, k, s):
        here = shard(t, place(k) + r, s, k)
        return remote(here, here, send_x.at[t, k, s], recv_x.at[t, k, s], rep=1 - r)

    def x_arrival(t, k, s):
        here = shard(t, place(k) + 1 - r, s, k)
        return remote(here, here, send_x.at[t, k, s], recv_x.at[t, k, s], rep=1 - r)

    def home_copy(t, q):
        return remote(hbm[t].at[n_local - 2 + q], shard(t, q, z, 1), home_send.at[t, q], home_recv.at[t, q], ep=y_peer)

    def send_own(k, t, own=True):
        @pl.when(z > 0)
        def _():
            for u in parts(k, t):
                z_copy(u, k, z, False, own).start()

        @pl.when(z < N_Z - 1)
        def _():
            for u in parts(k, t):
                z_copy(u, k, z, True, own).start()

    def signal_neighbours(sem, peers):
        for peer in peers:
            pl.semaphore_signal(sem, inc=1, device_id={'ep': peer}, device_id_type=MESH)
        pl.semaphore_signal(sem, inc=1, device_id={'rep': 1 - r}, device_id_type=MESH)

        @pl.when(z > 0)
        def _():
            pl.semaphore_signal(sem, inc=1, device_id={'fsdp': (z + N_Z - 1) % N_Z}, device_id_type=MESH)

        @pl.when(z < N_Z - 1)
        def _():
            pl.semaphore_signal(sem, inc=1, device_id={'fsdp': (z + 1) % N_Z}, device_id_type=MESH)

    def event(k, j):
        dist, t = (j % 3 + 1, j // 3) if is_peer(k) else (j // 3 + 1, j % 3)
        left = (z + N_Z - dist) % N_Z
        right = (z + dist) % N_Z
        for u in parts(k, t):
            @pl.when(z + dist < N_Z)
            def _():
                z_copy(u, k, right, False, False).wait_recv()

                @pl.when(z > 0)
                def _():
                    z_copy(u, k, right, False, False).start()
                x_copy(u, k, right).start()

            @pl.when(z >= dist)
            def _():
                z_copy(u, k, left, True, False).wait_recv()

                @pl.when(z < N_Z - 1)
                def _():
                    z_copy(u, k, left, True, False).start()
                x_copy(u, k, left).start()

        last_packets = isinstance(k, int) and k >= n_packet - 1
        for t in range(3):
            if not last_packets and OWN_AFTER[t] == j:
                send_own(k + 1, t)
            if last_packets and PEER_OWN_AFTER[t] == (k - n_packet + 1) * N_EVENT + j:
                for q in range(2):
                    home_copy(t, q).wait_recv()
                send_own(n_packet, t, False)

    def wait_x(k, tensors=(0, 1, 2)):
        for dist in range(1, N_Z):
            for t in [u for t in tensors for u in parts(k, t)]:
                x_arrival(t, k, (z + dist) % N_Z).wait_recv()

    barrier = pltpu.get_barrier_semaphore()
    signal_neighbours(barrier, (core_peer, y_peer, far_peer))

    own_w = [pltpu.make_async_copy(hbm[t].at[e], shard(t, e, z, 1), own_sem.at[t, e])
             for e in range(n_local) for t in range(3)]
    own_x = pltpu.make_async_copy(x_hbm, toks.at[3], own_sem.at[3, 0])
    own_ids = pltpu.make_async_copy(ids_hbm, ids.at[3], own_sem.at[3, 1])
    own_gates = pltpu.make_async_copy(gates_hbm, gates.at[3], own_sem.at[3, 2])
    own_copies = own_w + [own_x, own_ids, own_gates]
    for copy in own_copies:
        copy.start()

    z_peers = (z + N_Z - 1) // N_Z + (2 * N_Z - 2 - z) // N_Z
    pl.semaphore_wait(barrier, 4 + z_peers)

    for t in range(3):
        send_own(0, t)
    meta = []
    for slot, peer in ((2, core_peer), (1, y_peer), (0, far_peer)):
        meta.append(remote(ids_hbm, ids.at[slot], meta_send.at[0, slot], meta_recv.at[0, slot], ep=peer))
        meta.append(remote(gates_hbm, gates.at[slot], meta_send.at[1, slot], meta_recv.at[1, slot], ep=peer))
    for copy in meta:
        copy.start()
    tok_core = remote(x_hbm, toks.at[2], tok_send.at[2], tok_recv.at[2], ep=core_peer)
    tok_y = remote(x_hbm, toks.at[1], tok_send.at[1], tok_recv.at[1], ep=y_peer)
    tok_far = remote(toks.at[1], toks.at[0], tok_send.at[0], tok_recv.at[0], ep=core_peer)
    tok_core.start()
    tok_y.start()

    def zero(i, carry):
        rows = pl.ds(pl.multiple_of(i % N_BLOCK * block, block), block)
        acc[i // N_BLOCK, rows, :] = jnp.zeros((block, acc.shape[2]), jnp.float32)
        return carry

    lax.fori_loop(0, 4 * N_BLOCK, zero, 0)

    for j in range(N_EVENT):
        event(0, j)
    for copy in own_copies:
        copy.wait()
    tok_y.wait_recv()
    tok_far.start()
    for copy in meta:
        copy.wait_recv()
    tok_core.wait_recv()
    for j in range(LEAD):
        event(1, j)
    wait_x(0)
    tok_far.wait_recv()

    def hidden(e, slot, rows):
        x = toks[slot, rows, :]
        a = jnp.dot(x, wg[e], preferred_element_type=jnp.float32)
        b = jnp.dot(x, wu[e], preferred_element_type=jnp.float32)
        return (a * jax.nn.sigmoid(a) * b).astype(jnp.bfloat16)

    def add_output(h, w_down, expert, slot, rows, start, width):
        o = jnp.dot(h, w_down, preferred_element_type=jnp.float32).astype(jnp.bfloat16).astype(jnp.float32)
        chosen = jnp.where(ids[slot, :, rows] == expert, gates[slot, :, rows], 0.0)
        gate = jnp.sum(chosen, axis=0, keepdims=True)
        gate = jnp.broadcast_to(gate, (128, h.shape[0])).T
        for c in range(width // 128):
            cols = pl.ds(start + c * 128, 128)
            acc[slot, rows, cols] += jnp.where(gate > 0, gate * o[:, c * 128:(c + 1) * 128], 0.0)

    def rows_of(row, block):
        return pl.ds(pl.multiple_of(row * block, block), block)

    def compute(e, slot, row, block):
        rows = rows_of(row, block)
        add_output(hidden(e, slot, rows), wd[e], p * n_local + e, slot, rows, 0, acc.shape[2])

    ffn = wg.shape[2]

    def peer_hidden(e, slot, row):
        rows = rows_of(row, block)
        toks[slot - 2, rows, pl.ds(pl.multiple_of(e * ffn, ffn), ffn)] = hidden(e, slot, rows)

    def peer_output(e, slot, n):
        start = pl.multiple_of(shard_at(n) * d_shard, d_shard)
        h = toks[slot - 2, :, pl.ds(pl.multiple_of(e * ffn, ffn), ffn)]
        expert = y_peer * n_local + n_local - 2 + e
        add_output(h, wd[e, :, pl.ds(start, d_shard)], expert, slot, pl.ds(0, n_tok), start, d_shard)

    def shard_at(n):
        odd, upper = z % 2, z // 2
        return (z, 1 + odd + 2 * upper - 2 * odd * upper, 2 - 2 * odd - upper + 2 * odd * upper, 3 - 3 * upper)[n]

    def columns(n):
        return pl.ds(pl.multiple_of(shard_at(n) * d_shard, d_shard), d_shard)

    def drain(k, own=True, tensors=(0, 1, 2)):
        for t in [u for t in tensors for u in parts(k, t)]:
            @pl.when(z > 0)
            def _():
                z_copy(t, k, z, False, own).wait_send()

            @pl.when(z < N_Z - 1)
            def _():
                z_copy(t, k, z, True, own).wait_send()
            for dist in range(1, N_Z):
                left = (z + N_Z - dist) % N_Z
                right = (z + dist) % N_Z

                @pl.when((z + dist < N_Z) & (z > 0))
                def _():
                    z_copy(t, k, right, False, False).wait_send()

                @pl.when((z >= dist) & (z < N_Z - 1))
                def _():
                    z_copy(t, k, left, True, False).wait_send()
                x_copy(t, k, (z + dist) % N_Z).wait_send()

    def events(i, k, steps, first=0, offset=0):
        for j in range(first, N_EVENT):
            if steps[j] >= offset:
                @pl.when(i == steps[j] - offset)
                def _():
                    event(k, j)

    n_step = 4 * N_BLOCK * 2
    last = n_packet - 1

    def packet(k, carry):
        def step(i, carry):
            events(i, k + 1, STEP_OF, LEAD)

            @pl.when((k == 1) & (i == 2))
            def _():
                pl.semaphore_wait(free, 2 + z_peers)
                for t in range(3):
                    for q in range(2):
                        home_copy(t, q).start()
            compute(2 * k + i % 2, i // 2 // N_BLOCK, i // 2 % N_BLOCK, block)
            return carry

        lax.fori_loop(0, n_step, step, 0)

        @pl.when(k == 0)
        def _():
            for j in range(LEAD):
                event(2, j)
            wait_x(1)
            drain(0)
            signal_neighbours(free, (y_peer,))
        return carry

    lax.fori_loop(0, last - 1, packet, 0)

    tail = n_tok // N_TAIL

    def block_of(ref, row):
        return ref.at[pl.ds(row * tail, tail), :]

    def to_core(row):
        return remote(block_of(acc.at[0], row), block_of(from_core, row),
                      sum_send.at[0, row], sum_recv.at[0, row], ep=core_peer)

    def to_core_near(n):
        return remote(acc.at[2, :, columns(n)], from_core.at[:, columns(n)],
                      sum_send.at[2, n], sum_recv.at[2, n], ep=core_peer)

    def to_y(row):
        return remote(block_of(acc.at[1], row), block_of(from_y, row),
                      sum_send.at[1, row], sum_recv.at[1, row], ep=y_peer)

    def far_first(i, carry):
        events(i, last, STEP_OF_LAST)
        compute(2 * last - 2 + r, i % 2, i // 2, block)
        return carry

    lax.fori_loop(0, 2 * N_BLOCK, far_first, 0)
    wait_x(last - 1)

    def far_second(i, carry):
        events(i, last, STEP_OF_LAST, offset=2 * N_BLOCK)
        compute(2 * last - 1 - r, i % 2, i // 2, tail)
        for n in range(N_TAIL):
            @pl.when(i == 2 * n)
            def _():
                to_core(n).start()

            @pl.when(i == 2 * n + 1)
            def _():
                to_core(n).wait_recv()
                rows = slice(n * tail, (n + 1) * tail)
                acc[1, rows, :] += from_core[rows, :]
                to_y(n).start()
                pl.semaphore_signal(credit.at[n], inc=1, device_id={'ep': core_peer}, device_id_type=MESH)
        return carry

    lax.fori_loop(0, 2 * N_TAIL, far_second, 0)

    def near(i, carry):
        events(i, last, STEP_OF_LAST, offset=2 * N_BLOCK + 2 * N_TAIL)
        compute(2 * last - 2 + i % 2, 2 + i // 2 // N_BLOCK, i // 2 % N_BLOCK, block)
        return carry

    lax.fori_loop(0, 4 * N_BLOCK, near, 0)

    def drain_step(k, carry):
        drain(k)
        return carry

    lax.fori_loop(1, last, drain_step, 0)
    for j in range(LEAD):
        event(n_packet, j)
    wait_x(last)

    def home(i, carry):
        events(i, n_packet, STEP_OF_PEER, LEAD)
        compute(2 * last + i % 2, 2 + i // 2 // N_BLOCK, i // 2 % N_BLOCK, block)
        return carry

    lax.fori_loop(0, 4 * N_BLOCK, home, 0)
    for copy in meta + [tok_core, tok_y, tok_far]:
        copy.wait_send()

    def peer_first(i, carry):
        events(i, n_packet, STEP_OF_PEER, LEAD, offset=4 * N_BLOCK)
        peer_hidden(r, 2 + i // N_BLOCK, i % N_BLOCK)
        return carry

    lax.fori_loop(0, 2 * N_BLOCK, peer_first, 0)
    event(n_packet, 6)
    wait_x(n_packet, (0, 1))

    def peer_second(i, carry):
        events(i, n_packet, STEP_OF_PEER, 7, offset=6 * N_BLOCK)
        peer_hidden(1 - r, 2 + i // N_BLOCK, i % N_BLOCK)
        return carry

    lax.fori_loop(0, 2 * N_BLOCK, peer_second, 0)
    for n in range(N_TAIL):
        pl.semaphore_wait(credit.at[n], 1)

    def outputs(e, n, complete):
        def output(i, carry):
            peer_output(e, 2 + i, n)
            if complete:
                @pl.when(i == 0)
                def _():
                    to_core_near(n).start()
            return carry

        lax.fori_loop(0, 2, output, 0)

    def finish(n):
        to_core_near(n).wait_recv()
        cols = columns(n)
        y = toks[3, :, cols].astype(jnp.float32) + (acc[3, :, cols] + from_core[:, cols] + from_y[:, cols])
        out_ref[:, cols] = y.astype(jnp.bfloat16)

    def wait_down(n):
        for u in parts(n_packet, 2):
            x_arrival(u, n_packet, shard_at(n)).wait_recv()

    outputs(r, 0, False)
    outputs(1 - r, 0, True)
    outputs(r, 1, False)
    event(n_packet, N_EVENT - 1)
    wait_down(1)
    outputs(1 - r, 1, True)
    outputs(r, 2, False)
    outputs(r, 3, False)
    wait_down(2)
    outputs(1 - r, 2, True)
    wait_down(3)
    outputs(1 - r, 3, True)
    drain(last)
    drain(n_packet, False, (0, 1))
    for t in range(3):
        for q in range(2):
            home_copy(t, q).wait_send()
    for n in range(N_TAIL):
        to_y(n).wait_recv()
        to_core(n).wait_send()
        to_y(n).wait_send()
    for n in range(N_Z):
        finish(n)
    drain(n_packet, False, (2,))
    for n in range(N_Z):
        to_core_near(n).wait_send()


def solution(mesh):
    tok_spec = P(('rep', 'fsdp', 'ep'), None)

    def device_step(x_blk, ids_blk, gate_blk, wg_blk, wu_blk, wd_blk):
        n_tok, d_model = x_blk.shape
        n_choice = ids_blk.shape[1]
        n_local, d_shard, ffn = wg_blk.shape
        dma = pltpu.SemaphoreType.DMA
        n_packet = n_local // 2
        any_space = pl.BlockSpec(memory_space=pl.ANY)
        flops = 4 * n_tok * n_local * 6 * d_model * ffn
        return pl.pallas_call(
            moe_kernel,
            out_shape=pltpu.VMEM((n_tok, d_model), jnp.bfloat16),
            in_specs=[any_space] * 6,
            out_specs=pl.BlockSpec(memory_space=pltpu.VMEM),
            scratch_shapes=[
                pltpu.VMEM((n_local, d_model, ffn), jnp.bfloat16),
                pltpu.VMEM((n_local, d_model, ffn), jnp.bfloat16),
                pltpu.VMEM((n_local, ffn, d_model), jnp.bfloat16),
                pltpu.VMEM((4, n_tok, d_model), jnp.bfloat16),
                pltpu.VMEM((4, n_choice, n_tok), jnp.int32),
                pltpu.VMEM((4, n_choice, n_tok), jnp.float32),
                pltpu.VMEM((4, n_tok, d_model), jnp.float32),
                pltpu.VMEM((n_tok, d_model), jnp.float32),
                pltpu.VMEM((n_tok, d_model), jnp.float32),
                dma((4, n_local)),
                dma((4, n_packet + 1, N_Z)),
                dma((4, n_packet + 1, N_Z)),
                dma((4, n_packet + 1, N_Z)),
                dma((4, n_packet + 1, N_Z)),
                dma((4, n_packet + 1, N_Z)),
                dma((3,)),
                dma((3,)),
                dma((2, 3)),
                dma((2, 3)),
                dma((3, 2)),
                dma((3, 2)),
                pltpu.SemaphoreType.REGULAR,
                dma((3, N_TAIL)),
                dma((3, N_TAIL)),
                pltpu.SemaphoreType.REGULAR((N_TAIL,)),
            ],
            compiler_params=pltpu.CompilerParams(
                collective_id=0, has_side_effects=True, vmem_limit_bytes=62914560),
            cost_estimate=pl.CostEstimate(flops=flops, bytes_accessed=32 << 20, transcendentals=0),
            name='moe',
        )(x_blk, ids_blk.T, gate_blk.T, wg_blk, wu_blk, wd_blk)

    return jax.shard_map(
        device_step, mesh=mesh,
        in_specs=(tok_spec, tok_spec, tok_spec, P('ep', 'fsdp', None), P('ep', 'fsdp', None), P('ep', None, 'fsdp')),
        out_specs=tok_spec, check_vma=False)
```

```python
import functools

import jax
import jax.numpy as jnp
from jax import lax
from jax.experimental import pallas as pl
from jax.experimental.pallas import tpu as pltpu
from jax.sharding import PartitionSpec as P

MESH = pl.DeviceIdType.MESH
N_Z = 4
N_BLOCK = 2
N_TAIL = 4
N_EVENT = 9
LEAD = 2
N_PART = 1
STEP_OF = (0, 0, 3, 4, 6, 9, 12, 13, 15)
STEP_OF_LAST = (2, 5, 6, 6, 8, 11, 12, 15, 17)
STEP_OF_PEER = (0, 0, 1, 3, 5, 8, 12, 15, 17)
OWN_AFTER = (5, 6, 7)
PEER_OWN_AFTER = (6, 10, 13)


def moe_kernel(x_hbm, ids_hbm, gates_hbm, wg_hbm, wu_hbm, wd_hbm, out_ref,
               wg, wu, wd, toks, ids, gates, acc, from_core, from_y,
               own_sem, recv_z, recv_x, send_r, send_l, send_x,
               tok_send, tok_recv, meta_send, meta_recv, home_send, home_recv, free,
               sum_send, sum_recv, credit):
    r = lax.axis_index('rep')
    z = lax.axis_index('fsdp')
    p = lax.axis_index('ep')
    core = p % 2
    core_peer = p + 1 - 2 * core
    y_peer = (p + 2) % 4
    far_peer = (core_peer + 2) % 4
    n_local = wg_hbm.shape[0]
    n_packet = n_local // 2
    d_shard = wg_hbm.shape[1]
    n_tok = x_hbm.shape[0]
    block = n_tok // N_BLOCK

    hbm = (wg_hbm, wu_hbm, wd_hbm)

    def shard(t, e, s, k=0):
        start = pl.multiple_of(s * d_shard, d_shard)
        if is_peer(k) and t >= 2:
            part = wd.shape[1] // N_PART
            return wd.at[e, pl.ds((t - 2) * part, part), pl.ds(start, d_shard)]
        if t == 2:
            return wd.at[e, :, pl.ds(start, d_shard)]
        return (wg, wu)[t].at[e, pl.ds(start, d_shard), :]

    def is_peer(k):
        return isinstance(k, int) and k == n_packet

    def parts(k, t):
        return range(2, 2 + N_PART) if is_peer(k) and t == 2 else (t,)

    def remote(src, dst, send_sem, recv_sem, **where):
        return pltpu.make_async_remote_copy(src_ref=src, dst_ref=dst, send_sem=send_sem, recv_sem=recv_sem,
                                            device_id=where, device_id_type=MESH)

    def place(k):
        return 2 * (k % n_packet)

    def z_copy(t, k, s, right, own):
        here = shard(t, place(k) + r, s, k)
        src = hbm[t].at[place(k) + r] if own else here
        send = send_r if right else send_l
        to = (z + 1) % N_Z if right else (z + N_Z - 1) % N_Z
        return remote(src, here, send.at[t, k, s], recv_z.at[t, k, s], fsdp=to)

    def x_copy(t, k, s):
        here = shard(t, place(k) + r, s, k)
        return remote(here, here, send_x.at[t, k, s], recv_x.at[t, k, s], rep=1 - r)

    def x_arrival(t, k, s):
        here = shard(t, place(k) + 1 - r, s, k)
        return remote(here, here, send_x.at[t, k, s], recv_x.at[t, k, s], rep=1 - r)

    def home_copy(t, q):
        return remote(hbm[t].at[n_local - 2 + q], shard(t, q, z), home_send.at[t, q], home_recv.at[t, q], ep=y_peer)

    def send_own(k, t, own=True):
        @pl.when(z > 0)
        def _():
            for u in parts(k, t):
                z_copy(u, k, z, False, own).start()

        @pl.when(z < N_Z - 1)
        def _():
            for u in parts(k, t):
                z_copy(u, k, z, True, own).start()

    def signal_neighbours(sem, peers):
        for peer in peers:
            pl.semaphore_signal(sem, inc=1, device_id={'ep': peer}, device_id_type=MESH)
        pl.semaphore_signal(sem, inc=1, device_id={'rep': 1 - r}, device_id_type=MESH)

        @pl.when(z > 0)
        def _():
            pl.semaphore_signal(sem, inc=1, device_id={'fsdp': (z + N_Z - 1) % N_Z}, device_id_type=MESH)

        @pl.when(z < N_Z - 1)
        def _():
            pl.semaphore_signal(sem, inc=1, device_id={'fsdp': (z + 1) % N_Z}, device_id_type=MESH)

    def event(k, j):
        dist, t = (j % 3 + 1, j // 3) if is_peer(k) else (j // 3 + 1, j % 3)
        left = (z + N_Z - dist) % N_Z
        right = (z + dist) % N_Z
        for u in parts(k, t):
            @pl.when(z + dist < N_Z)
            def _():
                z_copy(u, k, right, False, False).wait_recv()

                @pl.when(z > 0)
                def _():
                    z_copy(u, k, right, False, False).start()
                x_copy(u, k, right).start()

            @pl.when(z >= dist)
            def _():
                z_copy(u, k, left, True, False).wait_recv()

                @pl.when(z < N_Z - 1)
                def _():
                    z_copy(u, k, left, True, False).start()
                x_copy(u, k, left).start()

        last_packets = isinstance(k, int) and k >= n_packet - 1
        for t in range(3):
            if not last_packets and OWN_AFTER[t] == j:
                send_own(k + 1, t)
            if last_packets and PEER_OWN_AFTER[t] == (k - n_packet + 1) * N_EVENT + j:
                for q in range(2):
                    home_copy(t, q).wait_recv()
                send_own(n_packet, t, False)

    def wait_x(k, tensors=(0, 1, 2)):
        for dist in range(1, N_Z):
            for t in tensors:
                x_arrival(t, k, (z + dist) % N_Z).wait_recv()

    barrier = pltpu.get_barrier_semaphore()
    signal_neighbours(barrier, (core_peer, y_peer, far_peer))

    own_w = [pltpu.make_async_copy(hbm[t].at[e], shard(t, e, z), own_sem.at[t, e])
             for e in range(n_local) for t in range(3)]
    own_x = pltpu.make_async_copy(x_hbm, toks.at[3], own_sem.at[3, 0])
    own_ids = pltpu.make_async_copy(ids_hbm, ids.at[3], own_sem.at[3, 1])
    own_gates = pltpu.make_async_copy(gates_hbm, gates.at[3], own_sem.at[3, 2])
    own_copies = own_w + [own_x, own_ids, own_gates]
    for copy in own_copies:
        copy.start()

    z_peers = (z + N_Z - 1) // N_Z + (2 * N_Z - 2 - z) // N_Z
    pl.semaphore_wait(barrier, 4 + z_peers)

    for t in range(3):
        send_own(0, t)
    meta = []
    for slot, peer in ((2, core_peer), (1, y_peer), (0, far_peer)):
        meta.append(remote(ids_hbm, ids.at[slot], meta_send.at[0, slot], meta_recv.at[0, slot], ep=peer))
        meta.append(remote(gates_hbm, gates.at[slot], meta_send.at[1, slot], meta_recv.at[1, slot], ep=peer))
    for copy in meta:
        copy.start()
    tok_core = remote(x_hbm, toks.at[2], tok_send.at[2], tok_recv.at[2], ep=core_peer)
    tok_y = remote(x_hbm, toks.at[1], tok_send.at[1], tok_recv.at[1], ep=y_peer)
    tok_far = remote(toks.at[1], toks.at[0], tok_send.at[0], tok_recv.at[0], ep=core_peer)
    tok_core.start()
    tok_y.start()

    def zero(i, carry):
        rows = pl.ds(pl.multiple_of(i % N_BLOCK * block, block), block)
        acc[i // N_BLOCK, rows, :] = jnp.zeros((block, acc.shape[2]), jnp.float32)
        return carry

    lax.fori_loop(0, 4 * N_BLOCK, zero, 0)

    for j in range(N_EVENT):
        event(0, j)
    for copy in own_copies:
        copy.wait()
    tok_y.wait_recv()
    tok_far.start()
    for copy in meta:
        copy.wait_recv()
    tok_core.wait_recv()
    for j in range(LEAD):
        event(1, j)
    wait_x(0)
    tok_far.wait_recv()

    def hidden(e, slot, rows):
        x = toks[slot, rows, :]
        a = jnp.dot(x, wg[e], preferred_element_type=jnp.float32)
        b = jnp.dot(x, wu[e], preferred_element_type=jnp.float32)
        return (a * jax.nn.sigmoid(a) * b).astype(jnp.bfloat16)

    def add_output(h, w_down, expert, slot, rows, start, width):
        o = jnp.dot(h, w_down, preferred_element_type=jnp.float32).astype(jnp.bfloat16).astype(jnp.float32)
        chosen = jnp.where(ids[slot, :, rows] == expert, gates[slot, :, rows], 0.0)
        gate = jnp.sum(chosen, axis=0, keepdims=True)
        gate = jnp.broadcast_to(gate, (128, h.shape[0])).T
        for c in range(width // 128):
            cols = pl.ds(start + c * 128, 128)
            acc[slot, rows, cols] += jnp.where(gate > 0, gate * o[:, c * 128:(c + 1) * 128], 0.0)

    def rows_of(row, block):
        return pl.ds(pl.multiple_of(row * block, block), block)

    def compute(e, slot, row, block):
        rows = rows_of(row, block)
        add_output(hidden(e, slot, rows), wd[e], p * n_local + e, slot, rows, 0, acc.shape[2])

    ffn = wg.shape[2]

    def peer_hidden(e, slot, row):
        rows = rows_of(row, block)
        toks[slot - 2, rows, pl.ds(pl.multiple_of(e * ffn, ffn), ffn)] = hidden(e, slot, rows)

    def peer_output(e, slot, n):
        start = pl.multiple_of(shard_at(n) * d_shard, d_shard)
        h = toks[slot - 2, :, pl.ds(pl.multiple_of(e * ffn, ffn), ffn)]
        expert = y_peer * n_local + n_local - 2 + e
        add_output(h, wd[e, :, pl.ds(start, d_shard)], expert, slot, pl.ds(0, n_tok), start, d_shard)

    def shard_at(n):
        odd, upper = z % 2, z // 2
        return (z, 1 + odd + 2 * upper - 2 * odd * upper, 2 - 2 * odd - upper + 2 * odd * upper, 3 - 3 * upper)[n]

    def columns(n):
        return pl.ds(pl.multiple_of(shard_at(n) * d_shard, d_shard), d_shard)

    def drain(k, own=True, tensors=(0, 1, 2)):
        for t in [u for t in tensors for u in parts(k, t)]:
            @pl.when(z > 0)
            def _():
                z_copy(t, k, z, False, own).wait_send()

            @pl.when(z < N_Z - 1)
            def _():
                z_copy(t, k, z, True, own).wait_send()
            for dist in range(1, N_Z):
                left = (z + N_Z - dist) % N_Z
                right = (z + dist) % N_Z

                @pl.when((z + dist < N_Z) & (z > 0))
                def _():
                    z_copy(t, k, right, False, False).wait_send()

                @pl.when((z >= dist) & (z < N_Z - 1))
                def _():
                    z_copy(t, k, left, True, False).wait_send()
                x_copy(t, k, (z + dist) % N_Z).wait_send()

    def events(i, k, steps, first=0, offset=0):
        for j in range(first, N_EVENT):
            if steps[j] >= offset:
                @pl.when(i == steps[j] - offset)
                def _():
                    event(k, j)

    n_step = 4 * N_BLOCK * 2
    last = n_packet - 1

    def packet(k, carry):
        def step(i, carry):
            events(i, k + 1, STEP_OF, LEAD)

            @pl.when((k == 1) & (i == 2))
            def _():
                pl.semaphore_wait(free, 2 + z_peers)
                for t in range(3):
                    for q in range(2):
                        home_copy(t, q).start()
            compute(2 * k + i % 2, i // 2 // N_BLOCK, i // 2 % N_BLOCK, block)
            return carry

        lax.fori_loop(0, n_step, step, 0)

        @pl.when(k == 0)
        def _():
            for j in range(LEAD):
                event(2, j)
            wait_x(1)
            drain(0)
            signal_neighbours(free, (y_peer,))
        return carry

    lax.fori_loop(0, last - 1, packet, 0)

    tail = n_tok // N_TAIL

    def block_of(ref, row):
        return ref.at[pl.ds(row * tail, tail), :]

    def to_core(row):
        return remote(block_of(acc.at[0], row), block_of(from_core, row),
                      sum_send.at[0, row], sum_recv.at[0, row], ep=core_peer)

    def to_core_near(n):
        return remote(acc.at[2, :, columns(n)], from_core.at[:, columns(n)],
                      sum_send.at[2, n], sum_recv.at[2, n], ep=core_peer)

    def to_y(row):
        return remote(block_of(acc.at[1], row), block_of(from_y, row),
                      sum_send.at[1, row], sum_recv.at[1, row], ep=y_peer)

    def far_first(i, carry):
        events(i, last, STEP_OF_LAST)
        compute(2 * last - 2 + r, i % 2, i // 2, block)
        return carry

    lax.fori_loop(0, 2 * N_BLOCK, far_first, 0)
    wait_x(last - 1)

    def far_second(i, carry):
        events(i, last, STEP_OF_LAST, offset=2 * N_BLOCK)
        compute(2 * last - 1 - r, i % 2, i // 2, tail)
        for n in range(N_TAIL):
            @pl.when(i == 2 * n)
            def _():
                to_core(n).start()

            @pl.when(i == 2 * n + 1)
            def _():
                to_core(n).wait_recv()
                rows = slice(n * tail, (n + 1) * tail)
                acc[1, rows, :] += from_core[rows, :]
                to_y(n).start()
                pl.semaphore_signal(credit.at[n], inc=1, device_id={'ep': core_peer}, device_id_type=MESH)
        return carry

    lax.fori_loop(0, 2 * N_TAIL, far_second, 0)

    def near(i, carry):
        events(i, last, STEP_OF_LAST, offset=2 * N_BLOCK + 2 * N_TAIL)
        compute(2 * last - 2 + i % 2, 2 + i // 2 // N_BLOCK, i // 2 % N_BLOCK, block)
        return carry

    lax.fori_loop(0, 4 * N_BLOCK, near, 0)

    def drain_step(k, carry):
        drain(k)
        return carry

    lax.fori_loop(1, last, drain_step, 0)
    for j in range(LEAD):
        event(n_packet, j)
    wait_x(last)

    def home(i, carry):
        events(i, n_packet, STEP_OF_PEER, LEAD)
        compute(2 * last + i % 2, 2 + i // 2 // N_BLOCK, i // 2 % N_BLOCK, block)
        return carry

    lax.fori_loop(0, 4 * N_BLOCK, home, 0)
    for copy in meta + [tok_core, tok_y, tok_far]:
        copy.wait_send()

    def peer_first(i, carry):
        events(i, n_packet, STEP_OF_PEER, LEAD, offset=4 * N_BLOCK)
        peer_hidden(r, 2 + i // N_BLOCK, i % N_BLOCK)
        return carry

    lax.fori_loop(0, 2 * N_BLOCK, peer_first, 0)
    event(n_packet, 6)
    wait_x(n_packet, (0, 1))

    def peer_second(i, carry):
        events(i, n_packet, STEP_OF_PEER, 7, offset=6 * N_BLOCK)
        peer_hidden(1 - r, 2 + i // N_BLOCK, i % N_BLOCK)
        return carry

    lax.fori_loop(0, 2 * N_BLOCK, peer_second, 0)
    for n in range(N_TAIL):
        pl.semaphore_wait(credit.at[n], 1)

    def outputs(e, n, complete):
        def output(i, carry):
            peer_output(e, 2 + i, n)
            if complete:
                @pl.when(i == 0)
                def _():
                    to_core_near(n).start()
            return carry

        lax.fori_loop(0, 2, output, 0)

    def finish(n):
        to_core_near(n).wait_recv()
        cols = columns(n)
        y = toks[3, :, cols].astype(jnp.float32) + (acc[3, :, cols] + from_core[:, cols] + from_y[:, cols])
        out_ref[:, cols] = y.astype(jnp.bfloat16)

    def wait_down(n):
        for u in parts(n_packet, 2):
            x_arrival(u, n_packet, shard_at(n)).wait_recv()

    outputs(r, 0, False)
    outputs(1 - r, 0, True)
    outputs(r, 1, False)
    event(n_packet, N_EVENT - 1)
    wait_down(1)
    outputs(1 - r, 1, True)
    outputs(r, 2, False)
    outputs(r, 3, False)
    wait_down(2)
    outputs(1 - r, 2, True)
    wait_down(3)
    outputs(1 - r, 3, True)
    drain(last)
    drain(n_packet, False, (0, 1))
    for t in range(3):
        for q in range(2):
            home_copy(t, q).wait_send()
    for n in range(N_TAIL):
        to_y(n).wait_recv()
        to_core(n).wait_send()
        to_y(n).wait_send()
    for n in range(N_Z):
        finish(n)
    drain(n_packet, False, (2,))
    for n in range(N_Z):
        to_core_near(n).wait_send()


def solution(mesh):
    tok_spec = P(('rep', 'fsdp', 'ep'), None)

    def device_step(x_blk, ids_blk, gate_blk, wg_blk, wu_blk, wd_blk):
        n_tok, d_model = x_blk.shape
        n_choice = ids_blk.shape[1]
        n_local, d_shard, ffn = wg_blk.shape
        dma = pltpu.SemaphoreType.DMA
        n_packet = n_local // 2
        any_space = pl.BlockSpec(memory_space=pl.ANY)
        flops = 4 * n_tok * n_local * 6 * d_model * ffn
        return pl.pallas_call(
            moe_kernel,
            out_shape=pltpu.VMEM((n_tok, d_model), jnp.bfloat16),
            in_specs=[any_space] * 6,
            out_specs=pl.BlockSpec(memory_space=pltpu.VMEM),
            scratch_shapes=[
                pltpu.VMEM((n_local, d_model, ffn), jnp.bfloat16),
                pltpu.VMEM((n_local, d_model, ffn), jnp.bfloat16),
                pltpu.VMEM((n_local, ffn, d_model), jnp.bfloat16),
                pltpu.VMEM((4, n_tok, d_model), jnp.bfloat16),
                pltpu.VMEM((4, n_choice, n_tok), jnp.int32),
                pltpu.VMEM((4, n_choice, n_tok), jnp.float32),
                pltpu.VMEM((4, n_tok, d_model), jnp.float32),
                pltpu.VMEM((n_tok, d_model), jnp.float32),
                pltpu.VMEM((n_tok, d_model), jnp.float32),
                dma((4, n_local)),
                dma((2 + N_PART, n_packet + 1, N_Z)),
                dma((2 + N_PART, n_packet + 1, N_Z)),
                dma((2 + N_PART, n_packet + 1, N_Z)),
                dma((2 + N_PART, n_packet + 1, N_Z)),
                dma((2 + N_PART, n_packet + 1, N_Z)),
                dma((3,)),
                dma((3,)),
                dma((2, 3)),
                dma((2, 3)),
                dma((3, 2)),
                dma((3, 2)),
                pltpu.SemaphoreType.REGULAR,
                dma((3, N_TAIL)),
                dma((3, N_TAIL)),
                pltpu.SemaphoreType.REGULAR((N_TAIL,)),
            ],
            compiler_params=pltpu.CompilerParams(
                collective_id=0, has_side_effects=True, vmem_limit_bytes=62914560),
            cost_estimate=pl.CostEstimate(flops=flops, bytes_accessed=32 << 20, transcendentals=0),
            name='moe',
        )(x_blk, ids_blk.T, gate_blk.T, wg_blk, wu_blk, wd_blk)

    return jax.shard_map(
        device_step, mesh=mesh,
        in_specs=(tok_spec, tok_spec, tok_spec, P('ep', 'fsdp', None), P('ep', 'fsdp', None), P('ep', None, 'fsdp')),
        out_specs=tok_spec, check_vma=False)
```
